128 devices in a mesh: gx: 8 (over z, core), yz: 16 (over y, x).
Axes of the slice: x: 4, y: 4, z: 4, core: 2. Of those that a mesh axis runs over, the one named last changes fastest.
Arguments:
- brick_ids: int32 [16384, 1], P(('gx', 'yz')), may hold values from 0 to 127; in each aligned block of 128 rows (0 to 127, 128 to 255, ...) at most 2 rows name the same one
- voxel_offset: int32 [16384, 256], P(('gx', 'yz')), may hold values from 0 to 4095
- fractions: float32 [16384, 3, 256], P(('gx', 'yz')), may hold values from 0 to 1
- normals: float32 [16384, 3, 256], P(('gx', 'yz')), may hold values from -6 to 6
- point_weight: float32 [16384, 256], P(('gx', 'yz')), may hold values from 0.1 to 10
- tile_count: int32 [128], P(('gx', 'yz')), may hold values from 96 to 128, as said below
Outputs:
- rhs: float32 [32, 128, 128], P('gx', 'yz')
- screen: float32 [32, 128, 128], P('gx', 'yz')
The draws below stay inside these ranges and needn't reach their ends.
Inputs may be any that keep to these rules, and one draw needn't show every extreme that they name: `brick_ids`: brick b belongs to index b // 16 of gx and b % 16 of yz. Among the 128 tile slots of one device no brick is named more than 2 times. `tile_count`: some device has all its slots valid in every draw.
All inputs are finite; a program needn't handle non-finite values.
Results may differ from the reference program's by a relative error of at most 0.0039.
Values sent between devices are 32-bit elements; how exact they have to be, the bound alone decides.
A program may use at most 64 MiB of HBM per device.

```python
import math
import jax
import jax.numpy as jnp
import numpy as np
from jax import lax

BX = 4
BY = 8
BZ = 128
TILE = 256
TILES_DEV = 128
CAP = 2
TILES = 16384
NX = 32
NY = 128
NZ = 128
N_YZ = 16
DEVICES = 128


def draw_tile_count(key, part):
    first = jax.random.fold_in(key, 11)
    second = jax.random.fold_in(key, 23)
    counts = jax.random.randint(first, (DEVICES,), max(1, 3 * TILES_DEV // 4), TILES_DEV + 1)
    filled = jax.random.randint(second, (), 0, DEVICES)
    return counts.at[filled].set(TILES_DEV).astype(jnp.int32)


def place_ends(entries, stream_key, least, high):
    longest = entries.shape.index(max(entries.shape))
    spots = []
    for shift in (0, 1):
        where = [jax.random.randint(jax.random.fold_in(stream_key, axis), (), 0, length) for axis, length in enumerate(entries.shape)]
        where[longest] = (where[longest] + shift) % entries.shape[longest]
        spots.append(tuple(where))
    return entries.at[spots[0]].set(least).at[spots[1]].set(high)


def level_of(rng, shape, cuts, low, top_value):
    factor_of = 1.0
    for dim, blocks in cuts:
        draws = jax.random.uniform(jax.random.fold_in(jax.random.fold_in(rng, 6), dim), (blocks,), jnp.float32, low / len(cuts), top_value / len(cuts))
        factor_of = factor_of * jnp.repeat(jnp.exp(draws), shape[dim] // blocks).reshape((-1,) + (1,) * (len(shape) - 1 - dim))
    return factor_of


def deal_out(key, own, number, rows, count, top, reach, slope):
    sequence = jax.random.permutation(key, count)
    crowded, usual = shares(count, rows * top, reach, slope, True), shares(count, rows * top, reach, slope, False)
    places = jnp.arange(count)

    def named(tallies, turn):
        used = int((tallies > 0).sum())
        fixed = max(1, used // 4)
        shifted = fixed + (places - fixed + turn * (used - fixed)) % max(1, count - fixed)
        return jnp.zeros((count,), jnp.int32).at[sequence[jnp.where(places < fixed, places, shifted)]].set(jnp.asarray(tallies, jnp.int32))

    tallies = jnp.where(number % 4 == 0, named(crowded, number // 4), named(usual, number - number // 4 - 1))
    mixed = jax.random.permutation(jax.random.fold_in(own, 3), count)
    donor, sink = mixed[0:count // 2 * 2:2], mixed[1:count // 2 * 2:2]
    room = jnp.minimum(tallies[donor] - 1, reach - tallies[sink]) // 2
    room = jnp.where((donor == sequence[0]) | (sink == sequence[0]) | (tallies[sink] == 0), 0, jnp.maximum(room, 0))
    shifted = jax.random.randint(jax.random.fold_in(own, 4), (count // 2,), 0, 1 << 20) % (room + 1)
    tallies = tallies.at[donor].add(-shifted).at[sink].add(shifted)
    labels = jnp.searchsorted(jnp.cumsum(tallies), jnp.arange(rows * top), side="right").astype(jnp.int32)
    grid = labels.reshape(top, rows).T
    grid = grid[jax.random.permutation(jax.random.fold_in(own, 1), rows)]
    turn = jax.random.randint(jax.random.fold_in(own, 2), (rows, 1), 0, top)
    return jnp.take_along_axis(grid, (jnp.arange(top)[None, :] + turn) % top, axis=1)


def shares(amount, total, bound, skew, full):
    weights = [(1 << 20) // math.isqrt(standing ** skew) + 1 for standing in range(1, amount + 1)]
    largest = bound if full else min(bound, max(-(-total // amount), total * weights[0] // sum(weights)))
    least = 1 if total - largest >= amount - 1 else 0
    given, spare = [largest] + [least] * (amount - 1), total - largest - least * (amount - 1)
    while spare > 0:
        movable = [i for i in range(1, amount) if given[i] < largest] or [i for i in range(1, amount) if given[i] < bound]
        whole, budget = sum([weights[i] for i in movable]), spare
        for i in movable:
            more = min(bound - given[i], max(1, budget * weights[i] // whole), spare)
            given[i] = given[i] + more
            spare = spare - more
    return np.array(given)


def bell_draw(rng, shape, scale, most, cuts=(), kind=jnp.bfloat16):
    result = jax.random.normal(rng, shape, jnp.float32) * scale
    if len(cuts) > 0:
        result = level_of(rng, shape, cuts, -0.22, 0.18) * result
    return jnp.clip(result, min=-most, max=most).astype(kind)


def setup_inputs(seed: int = 0) -> dict:
    arg_keys = jax.random.split(jax.random.key(seed), 7)
    brick_ids_keys = jax.random.split(jax.random.fold_in(arg_keys[0], 1), TILES // TILES_DEV)
    brick_ids_turns = jax.random.permutation(jax.random.fold_in(arg_keys[0], 3), TILES // TILES_DEV)
    brick_ids = jax.vmap(lambda own, number: deal_out(jax.random.fold_in(arg_keys[0], 2), own, number, TILES_DEV, DEVICES, 1, CAP, 2))(brick_ids_keys, brick_ids_turns).reshape((TILES, 1))
    voxel_offset = place_ends(jax.random.randint(arg_keys[1], (TILES, TILE), 0, BX * BY * BZ), jax.random.fold_in(arg_keys[1], 1), 0, (BX * BY * BZ) - 1).astype(jnp.int32)
    fractions = jnp.clip(1.0 * jax.random.uniform(arg_keys[2], (TILES, 3, TILE), jnp.float32) ** level_of(arg_keys[2], (TILES, 3, TILE), ((0, 128),), -0.2, 0.2), 0.0, 1.0)
    normals = bell_draw(arg_keys[3], (TILES, 3, TILE), 1.0, 6.0, ((0, 128),), jnp.float32)
    point_weight = jnp.clip(jnp.exp(math.log(10.0) - 4.6051702 * jax.random.uniform(arg_keys[4], (TILES, TILE), jnp.float32) ** level_of(arg_keys[4], (TILES, TILE), ((0, 128),), -0.2, 0.2)), 0.1, 10.0)
    tile_count = draw_tile_count(jax.random.fold_in(arg_keys[6], 71), 0)
    return dict(brick_ids=brick_ids, voxel_offset=voxel_offset, fractions=fractions, normals=normals, point_weight=point_weight, tile_count=tile_count)


def spline(frac):
    weights = jnp.stack([0.5 * (1.0 - frac) ** 2, 0.75 - (frac - 0.5) ** 2, 0.5 * frac * frac])
    slopes = jnp.stack([frac - 1.0, 1.0 - 2.0 * frac, frac])
    return weights, slopes


def rounded(value):
    return value.astype(jnp.bfloat16).astype(jnp.float32)


def reference(brick_ids, voxel_offset, fractions, normals, point_weight, tile_count):
    pad_y = NY + 2
    pad_z = NZ + 2
    total = (NX + 2) * pad_y * pad_z
    dest_all = brick_ids[:, 0].reshape(DEVICES, TILES_DEV)
    off_all = voxel_offset.reshape(DEVICES, TILES_DEV, TILE)
    frac_all = fractions.reshape(DEVICES, TILES_DEV, 3, TILE)
    norm_all = normals.reshape(DEVICES, TILES_DEV, 3, TILE)
    weight_all = point_weight.reshape(DEVICES, TILES_DEV, TILE)
    stencil = jnp.arange(3, dtype=jnp.int32)

    def step(carry, items):
        rhs_flat, screen_flat = carry
        dest, offset, frac, normal, weight, count = items
        valid = (jnp.arange(TILES_DEV, dtype=jnp.int32) < count).astype(jnp.float32)[:, None]
        normal = normal * valid[:, None, :]
        weight = weight * valid
        cell_x = offset // (BY * BZ)
        cell_y = (offset // BZ) % BY
        cell_z = offset % BZ
        base_x = (dest // N_YZ)[:, None] * BX + cell_x
        base_y = (dest % N_YZ)[:, None] * BY + cell_y
        wx, gx = spline(frac[:, 0])
        wy, gy = spline(frac[:, 1])
        wz, gz = spline(frac[:, 2])
        nx = normal[:, 0]
        ny = normal[:, 1]
        nz = normal[:, 2]
        a12 = rounded(nx[None, None] * gx[:, None] * wy[None, :] + ny[None, None] * wx[:, None] * gy[None, :])
        a3 = rounded(nz[None, None] * wx[:, None] * wy[None, :])
        a_s = rounded(weight[None, None] * wx[:, None] * wy[None, :])
        zb = rounded(wz)
        zd = rounded(gz)
        rhs_terms = a12[:, :, None] * zb[None, None] + a3[:, :, None] * zd[None, None]
        screen_terms = a_s[:, :, None] * zb[None, None]
        index = ((base_x[None, None, None] + stencil[:, None, None, None, None]) * pad_y
                 + base_y[None, None, None] + stencil[None, :, None, None, None]) * pad_z \
            + cell_z[None, None, None] + stencil[None, None, :, None, None]
        index = index.astype(jnp.int32).ravel()
        rhs_flat = rhs_flat.at[index].add(rhs_terms.ravel())
        screen_flat = screen_flat.at[index].add(screen_terms.ravel())
        return (rhs_flat, screen_flat), None

    start = (jnp.zeros((total,), jnp.float32), jnp.zeros((total,), jnp.float32))
    (rhs_flat, screen_flat), _ = lax.scan(step, start, (dest_all, off_all, frac_all, norm_all, weight_all, tile_count))
    rhs = rhs_flat.reshape(NX + 2, pad_y, pad_z)[1:-1, 1:-1, 1:-1]
    screen = screen_flat.reshape(NX + 2, pad_y, pad_z)[1:-1, 1:-1, 1:-1]
    return (rhs, screen)
```

```python
import jax
import jax.numpy as jnp
from jax import lax
from jax.experimental import pallas as pl
from jax.experimental.pallas import tpu as pltpu
from jax.sharding import PartitionSpec as P

BX, BY, BZ = 4, 8, 128
PX, PY = 36, 152
U = 8

CZ0, CZ1, CZ2, WZ0, WZ1, WZ2, GZ0, GZ1, GZ2 = range(9)
CX, WX0, WX1, WX2, GX0, GX1, GX2 = range(9, 16)
CY, WY0, WY1, WY2, GY0, GY1, GY2 = range(16, 23)
QNX, QNY, QNZ, QS = range(23, 27)
NQ = 27


def spline(f):
    return ((0.5 * (1.0 - f) ** 2, 0.75 - (f - 0.5) ** 2, 0.5 * f * f),
            (f - 1.0, 1.0 - 2.0 * f, f))


def prepare(count, off_ref, frac_ref, norm_ref, s_ref, q_ref):
    tiles = off_ref.shape[0]

    def put(k, r, value):
        for h in range(2):
            q_ref[k, h, r, :] = value[:, h * 128:h * 128 + 128]

    def group(g, _):
        r = pl.ds(pl.multiple_of(g * 8, 8), 8)
        off = off_ref[r, :]
        row = g * 8 + lax.broadcasted_iota(jnp.int32, off.shape, 0)
        valid = (row < count).astype(jnp.float32)
        cz = (off & (BZ - 1)).astype(jnp.float32)
        put(CZ0, r, cz - 1.0)
        put(CZ1, r, cz)
        put(CZ2, r, cz + 1.0)
        put(CX, r, (off >> 10).astype(jnp.float32))
        put(CY, r, ((off >> 7) & (BY - 1)).astype(jnp.float32))
        for dim, w0, g0 in ((0, WX0, GX0), (1, WY0, GY0), (2, WZ0, GZ0)):
            w, s = spline(frac_ref[dim, r, :])
            for k in range(3):
                put(w0 + k, r, w[k])
                put(g0 + k, r, s[k])
        for k in range(3):
            put(QNX + k, r, norm_ref[k, r, :] * valid)
        put(QS, r, s_ref[r, :] * valid)
        return 0

    lax.fori_loop(0, tiles // 8, group, 0)


def ROW(q_ref, k, h, t):
    return q_ref[k, h, pl.ds(t, 8, stride=0), :]


def bc(row, n=8):
    return jnp.broadcast_to(row, (n, row.shape[1]))


def tile_build(t, q_ref):
    parts = [half_build(t, h, q_ref) for h in range(2)]
    return tuple(jnp.concatenate(p, 1) for p in zip(*parts))


def half_build(t, h, q_ref):
    def row(k):
        return ROW(q_ref, k, h, t)

    def half(k):
        r = row(k)
        return jnp.concatenate([r, r], 0).astype(jnp.bfloat16)

    n = 128
    lanes = (8, n)
    cz = [half(CZ0 + k) for k in range(3)]
    wz = [half(WZ0 + k) for k in range(3)]
    gz = [half(GZ0 + k) for k in range(3)]
    zero = jnp.zeros((16, n), jnp.bfloat16)
    zb, zd = [], []
    for i in range(BZ // 16):
        at = (lax.broadcasted_iota(jnp.int32, (16, n), 0) + 16 * i).astype(jnp.bfloat16)
        hit = [at == c for c in cz]
        zb.append(jnp.where(hit[0], wz[0], jnp.where(hit[1], wz[1], jnp.where(hit[2], wz[2], zero))))
        zd.append(jnp.where(hit[0], gz[0], jnp.where(hit[1], gz[1], jnp.where(hit[2], gz[2], zero))))
    zb = jnp.concatenate(zb, 0)
    zd = jnp.concatenate(zd, 0)

    at = lax.broadcasted_iota(jnp.int32, lanes, 0).astype(jnp.float32)
    zf = jnp.zeros(lanes, jnp.float32)

    def spread(c, w0, g0):
        hit = [at == c + float(k) for k in range(3)]
        out = []
        for base in (w0, g0):
            v = [row(base + k) for k in range(3)]
            out.append(jnp.where(hit[0], v[0], jnp.where(hit[1], v[1], jnp.where(hit[2], v[2], zf))))
        return out

    wx, gx = spread(row(CX), WX0, GX0)
    cy = row(CY)
    wy, gy = spread(cy, WY0, GY0)
    last, before = cy == float(BY - 1), cy == float(BY - 2)
    wy8 = jnp.where(last, row(WY1), jnp.where(before, row(WY2), zf))
    gy8 = jnp.where(last, row(GY1), jnp.where(before, row(GY2), zf))
    wy9 = jnp.where(last, row(WY2), zf)
    gy9 = jnp.where(last, row(GY2), zf)
    p12x = row(QNX) * gx
    p12y = row(QNY) * wx
    p3 = row(QNZ) * wx
    ps = row(QS) * wx
    a12, a3, a_s = [], [], []
    for x in range(BX + 2):
        r = slice(x, x + 1)
        a12.append(bc(p12x[r]) * wy + bc(p12y[r]) * gy)
        a3.append(bc(p3[r]) * wy)
        a_s.append(bc(ps[r]) * wy)
    for w, g in ((wy8, gy8), (wy9, gy9)):
        a12.append(p12x * w + p12y * g)
        a3.append(p3 * w)
        a_s.append(ps * w)
    lhs1 = jnp.concatenate(a12 + a_s, 0).astype(jnp.bfloat16)
    lhs2 = jnp.concatenate(a3, 0).astype(jnp.bfloat16)
    return lhs1, lhs2, zb, zd


def contract(lhs1, lhs2, zb, zd):
    nt = (((1,), (1,)), ((), ()))
    r1 = lax.dot_general(lhs1, zb, nt, preferred_element_type=jnp.float32)
    r2 = lax.dot_general(lhs2, zd, nt, preferred_element_type=jnp.float32)
    return r1[:64] + r2, r1[64:]


def add_in(b, res, out_ref):
    x0 = (b // 16) * BX
    y0 = (b % 16) * BY + 7
    for f in range(2):
        base = (f * PX + x0) * PY + y0
        for x in range(BX + 2):
            r = pl.ds(base + x * PY, 8)
            out_ref[r, :] += res[f][8 * x:8 * x + 8]
        for k in range(2):
            r = pl.ds(base + 8 + k, 8, stride=PY)
            out_ref[r, :] += res[f][48 + 8 * k:56 + 8 * k]


def splat_kernel(dest_ref, count_ref, off_ref, frac_ref, norm_ref, s_ref, out_ref, q_ref):
    count = count_ref[0]
    out_ref[...] = jnp.zeros_like(out_ref)
    prepare(count, off_ref, frac_ref, norm_ref, s_ref, q_ref)

    def body(i, _):
        ts = [i * U + u for u in range(U)]
        res = [contract(*tile_build(t, q_ref)) for t in ts]
        for t, r in zip(ts, res):
            add_in(dest_ref[t], r, out_ref)
        return 0

    lax.fori_loop(0, (count + U - 1) // U, body, 0)


def splat(dest, count, off, frac, norm, s):
    tiles, n = off.shape
    vm = pl.BlockSpec(memory_space=pltpu.VMEM)
    sm = pl.BlockSpec(memory_space=pltpu.SMEM)
    return pl.pallas_call(
        splat_kernel,
        out_shape=jax.ShapeDtypeStruct((2 * PX * PY, BZ), jnp.float32),
        in_specs=[sm, sm, vm, vm, vm, vm],
        out_specs=vm,
        scratch_shapes=[pltpu.VMEM((NQ, 2, tiles, 128), jnp.float32)],
        compiler_params=pltpu.CompilerParams(vmem_limit_bytes=40 << 20),
        name="splat",
    )(dest, count, off, jnp.transpose(frac, (1, 0, 2)), jnp.transpose(norm, (1, 0, 2)), s)


def shards(brick_ids, voxel_offset, fractions, normals, point_weight, tile_count):
    grid = splat(brick_ids[:, 0], tile_count, voxel_offset, fractions, normals, point_weight)
    slabs, columns = lax.axis_size("gx"), lax.axis_size("yz")
    grid = grid.reshape(2, PX, PY, BZ)[:, 1:1 + slabs * BX, BY:BY + columns * BY]
    chunks = grid.reshape(2, slabs, BX, columns, BY, BZ).transpose(1, 3, 0, 2, 4, 5)
    chunks = chunks.reshape(slabs * columns, 2, BX, BY, BZ)
    mine = lax.psum_scatter(chunks, ("gx", "yz"), scatter_dimension=0, tiled=True)[0]
    return mine[0], mine[1]


def solution(mesh):
    return jax.shard_map(
        shards,
        mesh=mesh,
        in_specs=(
            P(("gx", "yz"), None),
            P(("gx", "yz"), None),
            P(("gx", "yz"), None, None),
            P(("gx", "yz"), None, None),
            P(("gx", "yz"), None),
            P(("gx", "yz")),
        ),
        out_specs=(P("gx", "yz", None), P("gx", "yz", None)),
        check_vma=False,
    )
```

```python
import jax
import jax.numpy as jnp
from jax import lax
from jax.experimental import pallas as pl
from jax.experimental.pallas import tpu as pltpu
from jax.sharding import PartitionSpec as P

BX, BY, BZ = 4, 8, 128
PX, PY = 36, 152
U = 8

CZ0, CZ1, CZ2, WZ0, WZ1, WZ2, GZ0, GZ1, GZ2 = range(9)
CX, WX0, WX1, WX2, GX0, GX1, GX2 = range(9, 16)
CY, WY0, WY1, WY2, GY0, GY1, GY2 = range(16, 23)
QNX, QNY, QNZ, QS = range(23, 27)
NQ = 27


def spline(f):
    return ((0.5 * (1.0 - f) ** 2, 0.75 - (f - 0.5) ** 2, 0.5 * f * f),
            (f - 1.0, 1.0 - 2.0 * f, f))


def prepare(count, off_ref, frac_ref, norm_ref, s_ref, q_ref):
    tiles = off_ref.shape[0]

    def put(k, r, value):
        for h in range(2):
            q_ref[k, h, r, :] = value[:, h * 128:h * 128 + 128]

    def group(g, _):
        r = pl.ds(pl.multiple_of(g * 8, 8), 8)
        off = off_ref[r, :]
        row = g * 8 + lax.broadcasted_iota(jnp.int32, off.shape, 0)
        valid = (row < count).astype(jnp.float32)
        cz = (off & (BZ - 1)).astype(jnp.float32)
        put(CZ0, r, cz - 1.0)
        put(CZ1, r, cz)
        put(CZ2, r, cz + 1.0)
        put(CX, r, (off >> 10).astype(jnp.float32))
        put(CY, r, ((off >> 7) & (BY - 1)).astype(jnp.float32))
        for dim, w0, g0 in ((0, WX0, GX0), (1, WY0, GY0), (2, WZ0, GZ0)):
            w, s = spline(frac_ref[dim, r, :])
            for k in range(3):
                put(w0 + k, r, w[k])
                put(g0 + k, r, s[k])
        for k in range(3):
            put(QNX + k, r, norm_ref[k, r, :] * valid)
        put(QS, r, s_ref[r, :] * valid)
        return 0

    lax.fori_loop(0, tiles // 8, group, 0)


def ROW(q_ref, k, h, t):
    return q_ref[k, h, pl.ds(t, 8, stride=0), :]


def bc(row, n=8):
    return jnp.broadcast_to(row, (n, row.shape[1]))


def tile_build(t, q_ref):
    parts = [half_build(t, h, q_ref) for h in range(2)]
    return tuple(jnp.concatenate(p, 1) for p in zip(*parts))


def half_build(t, h, q_ref):
    def row(k):
        return ROW(q_ref, k, h, t)

    def half(k):
        r = row(k)
        return jnp.concatenate([r, r], 0).astype(jnp.bfloat16)

    n = 128
    lanes = (8, n)
    cz = [half(CZ0 + k) for k in range(3)]
    wz = [half(WZ0 + k) for k in range(3)]
    gz = [half(GZ0 + k) for k in range(3)]
    zero = jnp.zeros((16, n), jnp.bfloat16)
    zb, zd = [], []
    for i in range(BZ // 16):
        at = (lax.broadcasted_iota(jnp.int32, (16, n), 0) + 16 * i).astype(jnp.bfloat16)
        hit = [at == c for c in cz]
        zb.append(jnp.where(hit[0], wz[0], jnp.where(hit[1], wz[1], jnp.where(hit[2], wz[2], zero))))
        zd.append(jnp.where(hit[0], gz[0], jnp.where(hit[1], gz[1], jnp.where(hit[2], gz[2], zero))))
    zb = jnp.concatenate(zb, 0)
    zd = jnp.concatenate(zd, 0)

    at = lax.broadcasted_iota(jnp.int32, lanes, 0).astype(jnp.float32)
    zf = jnp.zeros(lanes, jnp.float32)

    def spread(c, w0, g0):
        hit = [at == c + float(k) for k in range(3)]
        out = []
        for base in (w0, g0):
            v = [row(base + k) for k in range(3)]
            out.append(jnp.where(hit[0], v[0], jnp.where(hit[1], v[1], jnp.where(hit[2], v[2], zf))))
        return out

    wx, gx = spread(row(CX), WX0, GX0)
    cy = row(CY)
    wy, gy = spread(cy, WY0, GY0)
    last, before = cy == float(BY - 1), cy == float(BY - 2)
    wy8 = jnp.where(last, row(WY1), jnp.where(before, row(WY2), zf))
    gy8 = jnp.where(last, row(GY1), jnp.where(before, row(GY2), zf))
    wy9 = jnp.where(last, row(WY2), zf)
    gy9 = jnp.where(last, row(GY2), zf)
    p12x = row(QNX) * gx
    p12y = row(QNY) * wx
    p3 = row(QNZ) * wx
    ps = row(QS) * wx
    a12, a3, a_s = [], [], []
    for x in range(BX + 2):
        r = slice(x, x + 1)
        a12.append(bc(p12x[r]) * wy + bc(p12y[r]) * gy)
        a3.append(bc(p3[r]) * wy)
        a_s.append(bc(ps[r]) * wy)
    for w, g in ((wy8, gy8), (wy9, gy9)):
        a12.append(p12x * w + p12y * g)
        a3.append(p3 * w)
        a_s.append(ps * w)
    lhs1 = jnp.concatenate(a12 + a_s, 0).astype(jnp.bfloat16)
    lhs2 = jnp.concatenate(a3, 0).astype(jnp.bfloat16)
    return lhs1, lhs2, zb, zd


def contract(lhs1, lhs2, zb, zd):
    nt = (((1,), (1,)), ((), ()))
    r1 = lax.dot_general(lhs1, zb, nt, preferred_element_type=jnp.float32)
    r2 = lax.dot_general(lhs2, zd, nt, preferred_element_type=jnp.float32)
    return r1[:64] + r2, r1[64:]


def add_in(b, res, out_ref):
    x0 = (b // 16) * BX
    y0 = (b % 16) * BY + 7
    for f in range(2):
        base = (f * PX + x0) * PY + y0
        for x in range(BX + 2):
            r = pl.ds(base + x * PY, 8)
            out_ref[r, :] += res[f][8 * x:8 * x + 8]
        for k in range(2):
            r = pl.ds(base + 8 + k, 8, stride=PY)
            out_ref[r, :] += res[f][48 + 8 * k:56 + 8 * k]


def splat_kernel(dest_ref, count_ref, off_ref, frac_ref, norm_ref, s_ref, out_ref, q_ref):
    count = count_ref[0]
    out_ref[...] = jnp.zeros_like(out_ref)
    prepare(count, off_ref, frac_ref, norm_ref, s_ref, q_ref)

    def body(i, _):
        ts = [i * U + u for u in range(U)]
        res = [contract(*tile_build(t, q_ref)) for t in ts]
        for t, r in zip(ts, res):
            add_in(dest_ref[t], r, out_ref)
        return 0

    lax.fori_loop(0, (count + U - 1) // U, body, 0)


def splat(dest, count, off, frac, norm, s):
    tiles, n = off.shape
    vm = pl.BlockSpec(memory_space=pltpu.VMEM)
    sm = pl.BlockSpec(memory_space=pltpu.SMEM)
    return pl.pallas_call(
        splat_kernel,
        out_shape=jax.ShapeDtypeStruct((2 * PX * PY, BZ), jnp.float32),
        in_specs=[sm, sm, vm, vm, vm, vm],
        out_specs=vm,
        scratch_shapes=[pltpu.VMEM((NQ, 2, tiles, 128), jnp.float32)],
        compiler_params=pltpu.CompilerParams(vmem_limit_bytes=40 << 20),
        name="splat",
    )(dest, count, off, jnp.transpose(frac, (1, 0, 2)), jnp.transpose(norm, (1, 0, 2)), s)


N = 4
MESH = pl.DeviceIdType.MESH


class Copies:
    def __init__(self, send_sems, recv_sems):
        self.send_sems, self.recv_sems = send_sems, recv_sems
        self.made = []

    def start(self, src, dst, device):
        i = len(self.made)
        copy = pltpu.make_async_remote_copy(
            src_ref=src, dst_ref=dst, send_sem=self.send_sems.at[i], recv_sem=self.recv_sems.at[i],
            device_id=device, device_id_type=MESH)
        copy.start()
        self.made.append(copy)
        return copy

    def finish(self):
        for copy in self.made:
            copy.wait_send()


def reduce_kernel(grid_ref, rhs_ref, screen_ref, pair_ref, sum_ref, xa, xb, xc, xr, ya, yb, yc, yr, za, zb, zc, zr,
                  sx, sy, sz, rx, ry, rz, send_sems, recv_sems, ready_sem):
    slab, column = lax.axis_index("gx"), lax.axis_index("yz")
    pz, core = slab // 2, slab % 2
    py, px = column // N, column % N

    def device(dz=0, dy=0, dx=0):
        return (((pz + dz) % N) * 2 + core, ((py + dy) % N) * N + (px + dx) % N)

    other = (pz * 2 + 1 - core, column)
    lines = [device(**{axis: k}) for axis in ("dz", "dy", "dx") for k in range(1, N)]

    barrier = pltpu.get_barrier_semaphore()
    for peer in [other] + lines:
        pl.semaphore_signal(barrier, inc=1, device_id=peer, device_id_type=MESH)
    pl.semaphore_wait(barrier, 1 + len(lines))

    copies = Copies(send_sems, recv_sems)

    def slab_rows(j, which):
        return pl.ds(1 + BX * (((pz + j) % N) * 2 + which), BX)

    order = (2, 1, 3, 0)
    pair = {}
    for j in order:
        pair[j] = copies.start(grid_ref.at[:, slab_rows(j, 1 - core), pl.ds(BY, 128), :], pair_ref.at[j], other)
    for peer in lines:
        pl.semaphore_signal(ready_sem, inc=1, device_id=peer, device_id_type=MESH)

    def data_x(j, h, d):
        return (j, slice(0, 3), slice(2 * h, 2 * h + 2), (px + d) % N)

    def data_y(j, h, d):
        return (j, slice(3, 6), (py + d) % N, slice(2 * h, 2 * h + 2))

    def data_z(j, h, d):
        return (d % N, 6 + h)

    parts = {"x": (data_x, "dx", xa, xb, xc, xr), "y": (data_y, "dy", ya, yb, yc, yr), "z": (data_z, "dz", za, zb, zc, zr)}
    first, second, third = {}, {}, {}

    def toward(name, way):
        return device(**{parts[name][1]: 1 if way == 0 else N - 1})

    def send_far(name, j):
        data, _, a, _, _, _ = parts[name]
        for way in range(2):
            first[name, j, way] = copies.start(sum_ref.at[data(j, way, 2)], a.at[j, way], toward(name, way))

    def send_near(name, j, ways=(0, 1)):
        data, _, _, b, _, _ = parts[name]
        for way in ways:
            second[name, j, way] = copies.start(sum_ref.at[data(j, 1 - way, 1 if way == 0 else N - 1)], b.at[j, way],
                                                toward(name, way))

    def relay(name, j):
        data, _, a, _, c, r = parts[name]
        for way in range(2):
            first[name, j, way].wait_recv()
            r[j, way] = a[j, way] + sum_ref[data(j, way, 1 if way == 0 else N - 1)]
            third[name, j, way] = copies.start(r.at[j, way], c.at[j, way], toward(name, way))

    for at, j in enumerate(order):
        pair[j].wait_recv()
        rows = 1 + BX * (((pz + j) % N) * 2 + core)
        for f in range(2):
            def add_plane(x, _, f=f, rows=rows, j=j):
                total = grid_ref[f, rows + x, pl.ds(BY, 128), :] + pair_ref[j, f, x]
                sum_ref[j, BX * f + x] = total.reshape(N, N, BY, BZ)
                return 0
            lax.fori_loop(0, BX, add_plane, 0)
        send_far("x", j)
        send_far("y", j)
        if j == 2:
            send_far("z", 0)
        send_near("x", j)
        send_near("y", j)
        if j == 1:
            send_near("z", 0, (0,))
        if j == 3:
            send_near("z", 0, (1,))
        if at >= 2:
            relay("x", order[at - 2])
            relay("y", order[at - 2])
        if at == 2:
            relay("z", 0)
    for j in order[2:]:
        relay("x", j)
        relay("y", j)

    pl.semaphore_wait(ready_sem, len(lines))

    def joined(name, j, own):
        _, _, _, b, c, _ = parts[name]
        for way in range(2):
            second[name, j, way].wait_recv()
            third[name, j, way].wait_recv()
        return [own(h) + c[j, h] + b[j, 1 - h] for h in range(2)]

    last = []
    for j in order:
        for name, data, s, r in (("x", data_x, sx, rx), ("y", data_y, sy, ry)):
            low, high = joined(name, j, lambda h: sum_ref[data(j, h, 0)])
            s[j, :, 0:2] = low
            s[j, :, 2:4] = high
            for m in (2, 1, 3, 0):
                if (j, m) == (0, 0):
                    continue
                if name == "x":
                    where = s.at[j, :, (py + m) % N]
                    peer = device(dz=j, dy=m)
                else:
                    where = s.at[j, :, (px + m) % N]
                    peer = device(dz=j, dx=m)
                last.append(copies.start(where, r.at[j, m], peer))
    low, high = joined("z", 0, lambda h: sum_ref[data_z(0, h, 0)])
    sz[0] = low
    sz[1] = high
    for j in order:
        for m in (2, 1, 3, 0):
            if (j, m) == (0, 0):
                continue
            last.append(copies.start(sz.at[:, (py + j) % N, (px + m) % N], rz.at[j, m], device(dy=j, dx=m)))
    for copy in last:
        copy.wait_recv()

    others = [(j, m) for j in range(N) for m in range(N) if (j, m) != (0, 0)]

    def total(own, r):
        for j, m in others:
            own = own + r[j, m]
        return own

    fx = total(sx[0, :, py], rx)
    fy = total(sy[0, :, px], ry)
    fz = total(sz[:, py, px], rz)
    rhs_ref[0:3] = fx
    rhs_ref[3] = fy[0]
    screen_ref[0:2] = fy[1:3]
    screen_ref[2:4] = fz
    copies.finish()


def reduce_grid(grid):
    vm = pl.BlockSpec(memory_space=pltpu.VMEM)
    f32 = jnp.float32
    half = pltpu.VMEM((N, 2, 3, 2, BY, BZ), f32)
    plane = pltpu.VMEM((1, 2, N, N, BY, BZ), f32)
    made = 4 + 2 * 24 + 6 + 45
    return pl.pallas_call(
        reduce_kernel,
        out_shape=[jax.ShapeDtypeStruct((BX, BY, BZ), f32)] * 2,
        in_specs=[vm],
        out_specs=[vm, vm],
        scratch_shapes=[
            pltpu.VMEM((N, 2, BX, 128, BZ), f32),
            pltpu.VMEM((N, 2 * BX, N, N, BY, BZ), f32),
            half, half, half, half, half, half, half, half, plane, plane, plane, plane,
            pltpu.VMEM((N, 3, N, BY, BZ), f32), pltpu.VMEM((N, 3, N, BY, BZ), f32), pltpu.VMEM((2, N, N, BY, BZ), f32),
            pltpu.VMEM((N, N, 3, BY, BZ), f32), pltpu.VMEM((N, N, 3, BY, BZ), f32), pltpu.VMEM((N, N, 2, BY, BZ), f32),
            pltpu.SemaphoreType.DMA((made,)),
            pltpu.SemaphoreType.DMA((made,)),
            pltpu.SemaphoreType.REGULAR,
        ],
        compiler_params=pltpu.CompilerParams(collective_id=0, has_side_effects=True, vmem_limit_bytes=24 << 20),
        name="reduce_grid",
    )(grid)


def shards(brick_ids, voxel_offset, fractions, normals, point_weight, tile_count):
    grid = splat(brick_ids[:, 0], tile_count, voxel_offset, fractions, normals, point_weight)
    return tuple(reduce_grid(grid.reshape(2, PX, PY, BZ)))


def solution(mesh):
    return jax.shard_map(
        shards,
        mesh=mesh,
        in_specs=(
            P(("gx", "yz"), None),
            P(("gx", "yz"), None),
            P(("gx", "yz"), None, None),
            P(("gx", "yz"), None, None),
            P(("gx", "yz"), None),
            P(("gx", "yz")),
        ),
        out_specs=(P("gx", "yz", None), P("gx", "yz", None)),
        check_vma=False,
    )
```

```python
import jax
import jax.numpy as jnp
from jax import lax
from jax.experimental import pallas as pl
from jax.experimental.pallas import tpu as pltpu
from jax.sharding import PartitionSpec as P

BX, BY, BZ = 4, 8, 128
PX, PY = 36, 152
U = 8
NONE = 128
SLOTS = 136

CZ0, CZ1, CZ2, WZ0, WZ1, WZ2, GZ0, GZ1, GZ2 = range(9)
CX, WX0, WX1, WX2, GX0, GX1, GX2 = range(9, 16)
CY, WY0, WY1, WY2, GY0, GY1, GY2 = range(16, 23)
QNX, QNY, QNZ, QS = range(23, 27)
NQ = 27


def spline(f):
    return ((0.5 * (1.0 - f) ** 2, 0.75 - (f - 0.5) ** 2, 0.5 * f * f),
            (f - 1.0, 1.0 - 2.0 * f, f))


def tile_build(t, q_ref):
    parts = [half_build(t, h, q_ref) for h in range(2)]
    return tuple(jnp.concatenate(p, 1) for p in zip(*parts))


def half_build(t, h, q_ref):
    def row(k):
        return q_ref[k, h, pl.ds(t, 8, stride=0), :]

    def pair(k):
        r = row(k)
        return jnp.concatenate([r, r], 0).astype(jnp.bfloat16)

    eight, sixteen = (8, 128), (16, 128)
    cz = [pair(CZ0 + k) for k in range(3)]
    wz = [pair(WZ0 + k) for k in range(3)]
    gz = [pair(GZ0 + k) for k in range(3)]
    zero = jnp.zeros(sixteen, jnp.bfloat16)
    zb, zd = [], []
    for i in range(BZ // 16):
        at = (lax.broadcasted_iota(jnp.int32, sixteen, 0) + 16 * i).astype(jnp.bfloat16)
        hit = [at == c for c in cz]
        zb.append(jnp.where(hit[0], wz[0], jnp.where(hit[1], wz[1], jnp.where(hit[2], wz[2], zero))))
        zd.append(jnp.where(hit[0], gz[0], jnp.where(hit[1], gz[1], jnp.where(hit[2], gz[2], zero))))
    zb = jnp.concatenate(zb, 0)
    zd = jnp.concatenate(zd, 0)

    at = lax.broadcasted_iota(jnp.int32, eight, 0)
    at = [(at - k).astype(jnp.float32) for k in range(3)]
    none = jnp.zeros(eight, jnp.float32)

    def spread(c, w0, g0):
        hit = [a == c for a in at]
        out = []
        for base in (w0, g0):
            v = [row(base + k) for k in range(3)]
            out.append(jnp.where(hit[0], v[0], jnp.where(hit[1], v[1], jnp.where(hit[2], v[2], none))))
        return out

    wx, gx = spread(row(CX), WX0, GX0)
    cy = row(CY)
    wy, gy = spread(cy, WY0, GY0)
    last, before = cy == float(BY - 1), cy == float(BY - 2)
    wy8 = jnp.where(last, row(WY1), jnp.where(before, row(WY2), none))
    gy8 = jnp.where(last, row(GY1), jnp.where(before, row(GY2), none))
    wy9 = jnp.where(last, row(WY2), none)
    gy9 = jnp.where(last, row(GY2), none)
    p = (row(QNX) * gx, row(QNY) * wx, row(QNZ) * wx, row(QS) * wx)
    a12, a3, a_s = [], [], []
    for x in range(BX + 2):
        b = [jnp.broadcast_to(v[x:x + 1], eight) for v in p]
        a12.append(b[0] * wy + b[1] * gy)
        a3.append(b[2] * wy)
        a_s.append(b[3] * wy)
    for w, g in ((wy8, gy8), (wy9, gy9)):
        a12.append(p[0] * w + p[1] * g)
        a3.append(p[2] * w)
        a_s.append(p[3] * w)
    lhs1 = jnp.concatenate(a12 + a_s, 0).astype(jnp.bfloat16)
    lhs2 = jnp.concatenate(a3, 0).astype(jnp.bfloat16)
    return lhs1, lhs2, zb, zd


def contract(lhs1, lhs2, zb, zd):
    nt = (((1,), (1,)), ((), ()))
    r1 = lax.dot_general(lhs1, zb, nt, preferred_element_type=jnp.float32)
    r2 = lax.dot_general(lhs2, zd, nt, preferred_element_type=jnp.float32)
    return r1[:64] + r2, r1[64:]


def add_in(slab, column, res, out_ref):
    x0 = slab * BX
    y0 = column * BY + 7
    for f in range(2):
        base = (f * PX + x0) * PY + y0
        for x in range(BX + 2):
            r = pl.ds(base + x * PY, 8)
            out_ref[r, :] += res[f][8 * x:8 * x + 8]
        for k in range(2):
            r = pl.ds(base + 8 + k, 8, stride=PY)
            out_ref[r, :] += res[f][48 + 8 * k:56 + 8 * k]


def prepare_kernel(dest_hbm, count_hbm, off_hbm, frac_hbm, norm_hbm, s_hbm, grid_ref, q_ref, first_ref,
                   dest_ref, count_ref, off_ref, frac_ref, norm_ref, s_ref, list_ref, sems):
    pairs = ((count_hbm, count_ref), (dest_hbm, dest_ref), (off_hbm, off_ref), (frac_hbm, frac_ref), (norm_hbm, norm_ref),
             (s_hbm, s_ref))
    loads = [pltpu.make_async_copy(src, dst, sems.at[i]) for i, (src, dst) in enumerate(pairs)]
    for load in loads:
        load.start()
    grid_ref[...] = jnp.zeros_like(grid_ref)
    q_ref[:, :, pl.ds(NONE, 8), :] = jnp.zeros((NQ, 2, 8, 128), jnp.float32)

    def clear(i, _):
        for k in range(8):
            first_ref[i * 8 + k] = NONE
        return 0

    lax.fori_loop(0, NONE // 8, clear, 0)
    for load in loads:
        load.wait()
    count = count_ref[0]

    def group(g, seconds):
        r = pl.ds(pl.multiple_of(g * 8, 8), 8)

        def put(k, value):
            for h in range(2):
                q_ref[k, h, r, :] = value[:, h * 128:h * 128 + 128]

        off = off_ref[r, :]
        valid = g * 8 + lax.broadcasted_iota(jnp.int32, off.shape, 0) < count
        cz = (off & (BZ - 1)).astype(jnp.float32)
        put(CZ0, cz - 1.0)
        put(CZ1, cz)
        put(CZ2, cz + 1.0)
        put(CX, (off >> 10).astype(jnp.float32))
        put(CY, ((off >> 7) & (BY - 1)).astype(jnp.float32))
        for dim, w0, g0 in ((0, WX0, GX0), (1, WY0, GY0), (2, WZ0, GZ0)):
            w, s = spline(frac_ref[dim, r, :])
            for k in range(3):
                put(w0 + k, w[k])
                put(g0 + k, s[k])
        for k in range(3):
            put(QNX + k, jnp.where(valid, norm_ref[k, r, :], 0.0))
        put(QS, jnp.where(valid, s_ref[r, :], 0.0))
        for k in range(8):
            t = g * 8 + k
            brick = dest_ref[t]
            known = first_ref[brick]
            real = t < count
            again = jnp.logical_and(real, known < NONE)
            first_ref[brick] = jnp.where(jnp.logical_and(real, known == NONE), t, known)
            list_ref[seconds] = t
            seconds = seconds + again.astype(jnp.int32)
        return seconds

    seconds = lax.fori_loop(0, NONE // 8, group, 0)
    for k in range(U):
        list_ref[seconds + k] = NONE

    def more(i, _):
        ts = [list_ref[i * U + u] for u in range(U)]
        sums = [contract(*tile_build(t, q_ref)) for t in ts]
        for t, each in zip(ts, sums):
            brick = dest_ref[jnp.minimum(t, NONE - 1)]
            add_in(brick // 16, brick % 16, each, grid_ref)
        return 0

    lax.fori_loop(0, (seconds + U - 1) // U, more, 0)


def prepare(dest, count, off, frac, norm, s):
    tiles, n = off.shape
    hbm = pl.BlockSpec(memory_space=pltpu.HBM)
    f32 = jnp.float32
    return pl.pallas_call(
        prepare_kernel,
        out_shape=[jax.ShapeDtypeStruct((2 * PX * PY, BZ), f32), jax.ShapeDtypeStruct((NQ, 2, SLOTS, 128), f32),
                   jax.ShapeDtypeStruct((tiles,), jnp.int32)],
        in_specs=[hbm] * 6,
        out_specs=[pl.BlockSpec(memory_space=pltpu.VMEM)] * 2 + [pl.BlockSpec(memory_space=pltpu.SMEM)],
        scratch_shapes=[
            pltpu.SMEM((tiles,), jnp.int32), pltpu.SMEM((1,), jnp.int32), pltpu.VMEM((tiles, n), jnp.int32),
            pltpu.VMEM((3, tiles, n), f32), pltpu.VMEM((3, tiles, n), f32), pltpu.VMEM((tiles, n), f32),
            pltpu.SMEM((tiles + 2 * U,), jnp.int32), pltpu.SemaphoreType.DMA((6,)),
        ],
        compiler_params=pltpu.CompilerParams(vmem_limit_bytes=16 << 20),
        name="prepare",
    )(dest, count, off, jnp.transpose(frac, (1, 0, 2)), jnp.transpose(norm, (1, 0, 2)), s)


N = 4
MESH = pl.DeviceIdType.MESH


class Copies:
    def __init__(self, send_sems, recv_sems):
        self.send_sems, self.recv_sems = send_sems, recv_sems
        self.made = []

    def start(self, src, dst, device):
        i = len(self.made)
        copy = pltpu.make_async_remote_copy(
            src_ref=src, dst_ref=dst, send_sem=self.send_sems.at[i], recv_sem=self.recv_sems.at[i],
            device_id=device, device_id_type=MESH)
        copy.start()
        self.made.append(copy)
        return copy

    def finish(self):
        for copy in self.made:
            copy.wait_send()


def splat_kernel(first_ref, q_ref, start_ref, rhs_ref, screen_ref, grid_ref, pair_ref, sum_ref,
                 xa, xb, xc, xr, ya, yb, yc, yr, za, zb, zc, zr, sx, sy, sz, rx, ry, rz, send_sems, recv_sems, ready_sem):
    slab, column = lax.axis_index("gx"), lax.axis_index("yz")
    pz, core = slab // 2, slab % 2
    py, px = column // N, column % N

    def device(dz=0, dy=0, dx=0):
        return (((pz + dz) % N) * 2 + core, ((py + dy) % N) * N + (px + dx) % N)

    other = (pz * 2 + 1 - core, column)
    lines = [device(**{axis: k}) for axis in ("dz", "dy", "dx") for k in range(1, N)]
    barrier = pltpu.get_barrier_semaphore()
    for peer in [other] + lines:
        pl.semaphore_signal(barrier, inc=1, device_id=peer, device_id_type=MESH)

    flat = 2 * PX * PY

    def fetch(i, _):
        r = pl.ds(pl.multiple_of(i * 96, 96), 96)
        grid_ref[r, :] = start_ref[r, :]
        return 0

    lax.fori_loop(0, flat // 96, fetch, 0)

    def bricks(i, _):
        bx = (2 * pz + 3 + i // 2) % (2 * N)
        ys = [(i % 2) * U + u for u in range(U)]
        sums = [contract(*tile_build(first_ref[bx * 16 + y], q_ref)) for y in ys]
        for y, each in zip(ys, sums):
            add_in(bx, y, each, grid_ref)
        return 0

    copies = Copies(send_sems, recv_sems)
    grid = grid_ref.reshape(2, PX, PY, BZ)
    order = (2, 3, 0, 1)
    pair = {}

    def send_pair(j):
        rows = pl.ds(1 + BX * (((pz + j) % N) * 2 + 1 - core), BX)
        pair[j] = copies.start(grid.at[:, rows, pl.ds(BY, 128), :], pair_ref.at[j], other)

    def data_x(j, h, d):
        return (j, slice(0, 3), slice(2 * h, 2 * h + 2), (px + d) % N)

    def data_y(j, h, d):
        return (j, slice(3, 6), (py + d) % N, slice(2 * h, 2 * h + 2))

    def data_z(j, h, d):
        return (d % N, 6 + h)

    parts = {"x": (data_x, "dx", xa, xb, xc, xr), "y": (data_y, "dy", ya, yb, yc, yr), "z": (data_z, "dz", za, zb, zc, zr)}
    first, second, third = {}, {}, {}

    def toward(name, way):
        return device(**{parts[name][1]: 1 if way == 0 else N - 1})

    def send_far(name, j):
        data, _, a, _, _, _ = parts[name]
        for way in range(2):
            first[name, j, way] = copies.start(sum_ref.at[data(j, way, 2)], a.at[j, way], toward(name, way))

    def send_near(name, j, ways=(0, 1)):
        data, _, _, b, _, _ = parts[name]
        for way in ways:
            second[name, j, way] = copies.start(sum_ref.at[data(j, 1 - way, 1 if way == 0 else N - 1)], b.at[j, way],
                                                toward(name, way))

    def relay(name, j, ways=(0, 1)):
        data, _, a, _, c, r = parts[name]
        for way in ways:
            first[name, j, way].wait_recv()
            r[j, way] = a[j, way] + sum_ref[data(j, way, 1 if way == 0 else N - 1)]
            third[name, j, way] = copies.start(r.at[j, way], c.at[j, way], toward(name, way))

    def combine(j):
        pair[j].wait_recv()
        rows = 1 + BX * (((pz + j) % N) * 2 + core)
        for f in range(2):
            def add_plane(x, _, f=f):
                total = grid[f, rows + x, pl.ds(BY, 128), :] + pair_ref[j, f, x]
                sum_ref[j, BX * f + x] = total.reshape(N, N, BY, BZ)
                return 0
            lax.fori_loop(0, BX, add_plane, 0)
        send_far("x", j)
        send_far("y", j)
        if j == 2:
            send_far("z", 0)
        if j == 1:
            relay("z", 0, (0,))
            send_near("z", 0, (0,))
        if j == 3:
            send_near("z", 0, (1,))
        send_near("x", j)
        send_near("y", j)

    def joined(name, j, own):
        _, _, _, b, c, _ = parts[name]
        for way in range(2):
            second[name, j, way].wait_recv()
            third[name, j, way].wait_recv()
        return [own(h) + c[j, h] + b[j, 1 - h] for h in range(2)]

    last = []

    def owners(j):
        for name, data, s, r in (("x", data_x, sx, rx), ("y", data_y, sy, ry)):
            low, high = joined(name, j, lambda h: sum_ref[data(j, h, 0)])
            s[j, :, 0:2] = low
            s[j, :, 2:4] = high
            for m in (2, 1, 3, 0):
                if (j, m) == (0, 0):
                    continue
                if name == "x":
                    where, peer = s.at[j, :, (py + m) % N], device(dz=j, dy=m)
                else:
                    where, peer = s.at[j, :, (px + m) % N], device(dz=j, dx=m)
                last.append(copies.start(where, r.at[j, m], peer))

    lax.fori_loop(0, 8, bricks, 0)
    pl.semaphore_wait(barrier, 1 + len(lines))
    for peer in lines:
        pl.semaphore_signal(ready_sem, inc=1, device_id=peer, device_id_type=MESH)
    send_pair(2)
    lax.fori_loop(8, 12, bricks, 0)
    send_pair(3)
    combine(2)
    lax.fori_loop(12, 16, bricks, 0)
    send_pair(0)
    send_pair(1)
    combine(3)
    relay("x", 2)
    relay("y", 2)
    relay("z", 0, (1,))
    combine(0)
    relay("x", 3)
    relay("y", 3)
    combine(1)
    pl.semaphore_wait(ready_sem, len(lines))
    owners(2)
    relay("x", 0)
    relay("y", 0)
    owners(3)
    relay("x", 1)
    relay("y", 1)
    owners(0)
    low, high = joined("z", 0, lambda h: sum_ref[data_z(0, h, 0)])
    sz[0] = low
    sz[1] = high
    for j in order:
        for m in (2, 1, 3, 0):
            if (j, m) != (0, 0):
                last.append(copies.start(sz.at[:, (py + j) % N, (px + m) % N], rz.at[j, m], device(dy=j, dx=m)))
    owners(1)
    for copy in last:
        copy.wait_recv()

    def total(own, r):
        for j in range(N):
            for m in range(N):
                if (j, m) != (0, 0):
                    own = own + r[j, m]
        return own

    fx = total(sx[0, :, py], rx)
    fy = total(sy[0, :, px], ry)
    fz = total(sz[:, py, px], rz)
    rhs_ref[0:3] = fx
    rhs_ref[3] = fy[0]
    screen_ref[0:2] = fy[1:3]
    screen_ref[2:4] = fz
    copies.finish()


def splat(first, q, start):
    vm = pl.BlockSpec(memory_space=pltpu.VMEM)
    f32 = jnp.float32
    half = pltpu.VMEM((N, 2, 3, 2, BY, BZ), f32)
    plane = pltpu.VMEM((1, 2, N, N, BY, BZ), f32)
    made = 4 + 2 * 24 + 6 + 45
    return pl.pallas_call(
        splat_kernel,
        out_shape=[jax.ShapeDtypeStruct((BX, BY, BZ), f32)] * 2,
        in_specs=[pl.BlockSpec(memory_space=pltpu.SMEM), vm, vm],
        out_specs=[vm, vm],
        scratch_shapes=[
            pltpu.VMEM((2 * PX * PY, BZ), f32),
            pltpu.VMEM((N, 2, BX, 128, BZ), f32),
            pltpu.VMEM((N, 2 * BX, N, N, BY, BZ), f32),
            half, half, half, half, half, half, half, half, plane, plane, plane, plane,
            pltpu.VMEM((N, 3, N, BY, BZ), f32), pltpu.VMEM((N, 3, N, BY, BZ), f32), pltpu.VMEM((2, N, N, BY, BZ), f32),
            pltpu.VMEM((N, N, 3, BY, BZ), f32), pltpu.VMEM((N, N, 3, BY, BZ), f32), pltpu.VMEM((N, N, 2, BY, BZ), f32),
            pltpu.SemaphoreType.DMA((made,)),
            pltpu.SemaphoreType.DMA((made,)),
            pltpu.SemaphoreType.REGULAR,
        ],
        compiler_params=pltpu.CompilerParams(collective_id=0, has_side_effects=True, vmem_limit_bytes=28 << 20),
        name="splat",
    )(first, q, start)


def shards(brick_ids, voxel_offset, fractions, normals, point_weight, tile_count):
    grid, q, first = prepare(brick_ids[:, 0], tile_count, voxel_offset, fractions, normals, point_weight)
    return tuple(splat(first, q, grid))


def solution(mesh):
    return jax.shard_map(
        shards,
        mesh=mesh,
        in_specs=(
            P(("gx", "yz"), None),
            P(("gx", "yz"), None),
            P(("gx", "yz"), None, None),
            P(("gx", "yz"), None, None),
            P(("gx", "yz"), None),
            P(("gx", "yz")),
        ),
        out_specs=(P("gx", "yz", None), P("gx", "yz", None)),
        check_vma=False,
    )
```

```python
import jax
import jax.numpy as jnp
from jax import lax
from jax.experimental import pallas as pl
from jax.experimental.pallas import tpu as pltpu
from jax.sharding import PartitionSpec as P

BX, BY, BZ = 4, 8, 128
PX, PY = 36, 152
V = 8

CZ, WZ, GZ = 0, 3, 6
WY, GY = 9, 19
PXX, PXY, PXZ, PXS = 29, 37, 45, 53
HALF = 61
ROWS = 123
NONE = 128


def spline(f):
    return ((0.5 * (1.0 - f) ** 2, 0.75 - (f - 0.5) ** 2, 0.5 * f * f),
            (f - 1.0, 1.0 - 2.0 * f, f))


def slots(cell, cells, values):
    hit = [cell == c for c in range(cells)]
    out = []
    for i in range(cells + 2):
        total = 0.0
        for k in range(3):
            if 0 <= i - k < cells:
                total = jnp.where(hit[i - k], values[k], total)
        out.append(total)
    return out


def tile_build(t, q_ref):
    parts = [half_build(t * ROWS + h * HALF, q_ref) for h in range(2)]
    return tuple(jnp.concatenate(p, 1) for p in zip(*parts))


def half_build(base, q_ref):
    def row(k):
        return q_ref[pl.ds(base + k, 8, stride=0), :]

    def rows(k):
        return q_ref[pl.ds(base + k, 8), :]

    def pair(k):
        r = row(k)
        return jnp.concatenate([r, r], 0).astype(jnp.bfloat16)

    sixteen = (16, 128)
    cz = [pair(CZ + k) for k in range(3)]
    wz = [pair(WZ + k) for k in range(3)]
    gz = [pair(GZ + k) for k in range(3)]
    zero = jnp.zeros(sixteen, jnp.bfloat16)
    zb, zd = [], []
    for i in range(BZ // 16):
        at = (lax.broadcasted_iota(jnp.int32, sixteen, 0) + 16 * i).astype(jnp.bfloat16)
        hit = [at == c for c in cz]
        zb.append(jnp.where(hit[0], wz[0], jnp.where(hit[1], wz[1], jnp.where(hit[2], wz[2], zero))))
        zd.append(jnp.where(hit[0], gz[0], jnp.where(hit[1], gz[1], jnp.where(hit[2], gz[2], zero))))
    zb = jnp.concatenate(zb, 0)
    zd = jnp.concatenate(zd, 0)

    wy, gy = rows(WY), rows(GY)
    a12, a3, a_s = [], [], []
    for x in range(BX + 2):
        a12.append(row(PXX + x) * wy + row(PXY + x) * gy)
        a3.append(row(PXZ + x) * wy)
        a_s.append(row(PXS + x) * wy)
    p = [rows(k) for k in (PXX, PXY, PXZ, PXS)]
    for y in (BY, BY + 1):
        w, g = row(WY + y), row(GY + y)
        a12.append(p[0] * w + p[1] * g)
        a3.append(p[2] * w)
        a_s.append(p[3] * w)
    lhs1 = jnp.concatenate(a12 + a_s, 0).astype(jnp.bfloat16)
    lhs2 = jnp.concatenate(a3, 0).astype(jnp.bfloat16)
    return lhs1, lhs2, zb, zd


def contract(lhs1, lhs2, zb, zd):
    nt = (((1,), (1,)), ((), ()))
    r1 = lax.dot_general(lhs1, zb, nt, preferred_element_type=jnp.float32)
    r2 = lax.dot_general(lhs2, zd, nt, preferred_element_type=jnp.float32)
    return r1[:64] + r2, r1[64:]


def add_in(slab, column, res, out_ref):
    x0 = slab * BX
    y0 = column * BY + 7
    for f in range(2):
        base = (f * PX + x0) * PY + y0
        for x in range(BX + 2):
            r = pl.ds(base + x * PY, 8)
            out_ref[r, :] += res[f][8 * x:8 * x + 8]
        for k in range(2):
            r = pl.ds(base + 8 + k, 8, stride=PY)
            out_ref[r, :] += res[f][48 + 8 * k:56 + 8 * k]


def prepare_kernel(count_ref, dest_hbm, off_hbm, frac_hbm, norm_hbm, s_hbm, grid_ref, q_ref, first_ref,
                   dest_ref, off_ref, frac_ref, norm_ref, s_ref, list_ref, sems):
    pairs = ((dest_hbm, dest_ref), (off_hbm, off_ref), (frac_hbm, frac_ref), (norm_hbm, norm_ref),
             (s_hbm, s_ref))
    loads = [pltpu.make_async_copy(src, dst, sems.at[i]) for i, (src, dst) in enumerate(pairs)]
    for load in loads:
        load.start()
    grid_ref[...] = jnp.zeros_like(grid_ref)
    q_ref[pl.ds(NONE * ROWS, 128), :] = jnp.zeros((128, 128), jnp.float32)

    def clear(i, _):
        for k in range(8):
            first_ref[i * 8 + k] = NONE
        return 0

    lax.fori_loop(0, NONE // 8, clear, 0)
    for load in loads:
        load.wait()
    count = count_ref[0]

    def group(g, seconds):
        r = pl.ds(pl.multiple_of(g * 8, 8), 8)
        valid = g * 8 + lax.broadcasted_iota(jnp.int32, (8, 128), 0) < count
        for h in range(2):
            lanes = slice(h * 128, h * 128 + 128)

            def put(k, value):
                q_ref[pl.ds(g * 8 * ROWS + h * HALF + k, 8, stride=ROWS), :] = value

            off = off_ref[r, lanes]
            nx, ny, nz = (jnp.where(valid, norm_ref[k, r, lanes], 0.0) for k in range(3))
            s = jnp.where(valid, s_ref[r, lanes], 0.0)
            cell = off & (BZ - 1)
            w, slope = spline(frac_ref[2, r, lanes])
            for k in range(3):
                put(CZ + k, (cell + (k - 1)).astype(jnp.float32))
                put(WZ + k, w[k])
                put(GZ + k, slope[k])
            w, slope = spline(frac_ref[1, r, lanes])
            cell = (off >> 7) & (BY - 1)
            for base, values in ((WY, w), (GY, slope)):
                for i, value in enumerate(slots(cell, BY, values)):
                    put(base + i, value)
            w, slope = spline(frac_ref[0, r, lanes])
            cell = off >> 10
            wx, gx = slots(cell, BX, w), slots(cell, BX, slope)
            for i in range(BX + 2):
                put(PXX + i, nx * gx[i])
                put(PXY + i, ny * wx[i])
                put(PXZ + i, nz * wx[i])
                put(PXS + i, s * wx[i])
            none = jnp.zeros((8, 128), jnp.float32)
            for base in (PXX, PXY, PXZ, PXS):
                put(base + BX + 2, none)
                put(base + BX + 3, none)
        for k in range(8):
            t = g * 8 + k
            brick = dest_ref[t]
            known = first_ref[brick]
            real = t < count
            again = jnp.logical_and(real, known < NONE)
            first_ref[brick] = jnp.where(jnp.logical_and(real, known == NONE), t, known)
            list_ref[seconds] = t
            seconds = seconds + again.astype(jnp.int32)
        return seconds

    seconds = lax.fori_loop(0, NONE // 8, group, 0)
    for k in range(V):
        list_ref[seconds + k] = NONE

    def more(i, _):
        ts = [list_ref[i * V + u] for u in range(V)]
        sums = [contract(*tile_build(t, q_ref)) for t in ts]
        for t, each in zip(ts, sums):
            brick = dest_ref[jnp.minimum(t, NONE - 1)]
            add_in(brick // 16, brick % 16, each, grid_ref)
        return 0

    lax.fori_loop(0, (seconds + V - 1) // V, more, 0)


def prepare(dest, count, off, frac, norm, s):
    tiles, n = off.shape
    hbm = pl.BlockSpec(memory_space=pltpu.HBM)
    f32 = jnp.float32
    return pl.pallas_call(
        prepare_kernel,
        out_shape=[jax.ShapeDtypeStruct((2 * PX * PY, BZ), f32), jax.ShapeDtypeStruct((NONE * ROWS + 128, 128), f32),
                   jax.ShapeDtypeStruct((tiles,), jnp.int32)],
        in_specs=[pl.BlockSpec(memory_space=pltpu.SMEM)] + [hbm] * 5,
        out_specs=[pl.BlockSpec(memory_space=pltpu.VMEM)] * 2 + [pl.BlockSpec(memory_space=pltpu.SMEM)],
        scratch_shapes=[
            pltpu.SMEM((tiles,), jnp.int32), pltpu.VMEM((tiles, n), jnp.int32),
            pltpu.VMEM((3, tiles, n), f32), pltpu.VMEM((3, tiles, n), f32), pltpu.VMEM((tiles, n), f32),
            pltpu.SMEM((tiles + 2 * V,), jnp.int32), pltpu.SemaphoreType.DMA((5,)),
        ],
        compiler_params=pltpu.CompilerParams(vmem_limit_bytes=22 << 20),
        name="prepare",
    )(count, *(pltpu.with_memory_space_constraint(x, pltpu.HBM) for x in
               (dest, off, jnp.transpose(frac, (1, 0, 2)), jnp.transpose(norm, (1, 0, 2)), s)))


N = 4
MESH = pl.DeviceIdType.MESH


class Copies:
    def __init__(self, send_sems, recv_sems):
        self.send_sems, self.recv_sems = send_sems, recv_sems
        self.made = []

    def start(self, src, dst, device):
        i = len(self.made)
        copy = pltpu.make_async_remote_copy(
            src_ref=src, dst_ref=dst, send_sem=self.send_sems.at[i], recv_sem=self.recv_sems.at[i],
            device_id=device, device_id_type=MESH)
        copy.start()
        self.made.append(copy)
        return copy

    def finish(self):
        for copy in self.made:
            copy.wait_send()


PARTS = (3, 3, 2)


def splat_kernel(first_ref, q_ref, start_ref, rhs_ref, screen_ref, grid_ref, pair_ref, sum_ref,
                 xa, xb, xc, xr, ya, yb, yc, yr, za, zb, zc, zr, sx, sy, sz, rx, ry, rz, send_sems, recv_sems, ready_sem):
    slab, column = lax.axis_index("gx"), lax.axis_index("yz")
    pz, core = slab // 2, slab % 2
    py, px = column // N, column % N

    def device(dz=0, dy=0, dx=0):
        return (((pz + dz) % N) * 2 + core, ((py + dy) % N) * N + (px + dx) % N)

    other = (pz * 2 + 1 - core, column)
    lines = [device(**{axis: k}) for axis in ("dz", "dy", "dx") for k in range(1, N)]
    barrier = pltpu.get_barrier_semaphore()
    for peer in [other] + lines:
        pl.semaphore_signal(barrier, inc=1, device_id=peer, device_id_type=MESH)

    def fetch(i, _):
        r = pl.ds(pl.multiple_of(i * 96, 96), 96)
        grid_ref[r, :] = start_ref[r, :]
        return 0

    lax.fori_loop(0, 2 * PX * PY // 96, fetch, 0)

    def bricks(place):
        def step(i, _):
            ys = [(N * py + 2 * N + N * N + place(2 * i + k)) % (N * N) for k in range(2)]
            places = [(x, y) for y in ys for x in range(2 * N)]
            sums = [contract(*tile_build(first_ref[x * 16 + y], q_ref)) for x, y in places]
            for (x, y), each in zip(places, sums):
                add_in(x, y, each, grid_ref)
            return 0
        return step

    copies = Copies(send_sems, recv_sems)
    grid = grid_ref.reshape(2, PX, PY, BZ)
    pair = {}

    def rows_of(o):
        return pl.ds(pl.multiple_of(BY + N * BY * ((py + o) % N), BY), N * BY)

    def cells_of(j, which):
        return 1 + BX * (((pz + j) % N) * 2 + which)

    def send_pair(o):
        for j in range(N):
            pair[o, j] = copies.start(grid.at[:, pl.ds(cells_of(j, 1 - core), BX), rows_of(o), :], pair_ref.at[o, j], other)

    nx, ny, nz = PARTS
    xs, ys, zs = slice(0, nx), slice(nx, nx + ny), slice(nx + ny, nx + ny + nz)

    def data_x(o, h, d):
        return (o, slice(2 * h, 2 * h + 2), xs, (px + d) % N)

    def data_y(o, h, d):
        return (d % N, slice(2 * h, 2 * h + 2), ys)

    def data_z(o, h, d):
        return (o, d % N, zs, slice(2 * h, 2 * h + 2))

    parts = {"x": (data_x, "dx", xa, xb, xc, xr), "y": (data_y, "dy", ya, yb, yc, yr), "z": (data_z, "dz", za, zb, zc, zr)}
    first, second, third = {}, {}, {}

    def toward(name, way):
        return device(**{parts[name][1]: 1 if way == 0 else N - 1})

    def send_far(name, o):
        data, _, a, _, _, _ = parts[name]
        for way in range(2):
            first[name, o, way] = copies.start(sum_ref.at[data(o, way, 2)], a.at[o, way], toward(name, way))

    def send_near(name, o, ways=(0, 1)):
        data, _, _, b, _, _ = parts[name]
        for way in ways:
            second[name, o, way] = copies.start(sum_ref.at[data(o, 1 - way, 1 if way == 0 else N - 1)], b.at[o, way],
                                                toward(name, way))

    def relay(name, o, ways=(0, 1)):
        data, _, a, _, c, r = parts[name]
        for way in ways:
            first[name, o, way].wait_recv()
            r[o, way] = a[o, way] + sum_ref[data(o, way, 1 if way == 0 else N - 1)]
            third[name, o, way] = copies.start(r.at[o, way], c.at[o, way], toward(name, way))

    def combine(o):
        for j in range(N):
            pair[o, j].wait_recv()
            for f in range(2):
                for x in range(BX):
                    total = grid[f, cells_of(j, core) + x, rows_of(o), :] + pair_ref[o, j, f, x]
                    sum_ref[o, j, BX * f + x] = total.reshape(N, BY, BZ)
        send_far("x", o)
        send_far("z", o)
        if o == 2:
            send_far("y", 0)
        send_near("x", o)
        send_near("z", o)
        if o == 3:
            relay("y", 0, (1,))
            send_near("y", 0, (1,))
        if o == 1:
            relay("y", 0, (0,))
            send_near("y", 0, (0,))

    def joined(name, o, own):
        _, _, _, b, c, _ = parts[name]
        for way in range(2):
            second[name, o, way].wait_recv()
            third[name, o, way].wait_recv()
        return [own(h) + c[o, h] + b[o, 1 - h] for h in range(2)]

    last = []

    def owners(o):
        sx[o, 0:2], sx[o, 2:4] = joined("x", o, lambda h: sum_ref[data_x(o, h, 0)])
        sz[o, :, 0:2], sz[o, :, 2:4] = joined("z", o, lambda h: sum_ref[data_z(o, h, 0)])
        for k in (2, 1, 3, 0):
            if (o, k) != (0, 0):
                last.append(copies.start(sx.at[o, k], rx.at[o, k], device(dy=o, dz=k)))
                last.append(copies.start(sz.at[o, :, (px + k) % N], rz.at[o, k], device(dy=o, dx=k)))

    def owners_y():
        sy[0:2], sy[2:4] = joined("y", 0, lambda h: sum_ref[data_y(0, h, 0)])
        for j in (2, 1, 3, 0):
            for k in (2, 1, 3, 0):
                if (j, k) != (0, 0):
                    last.append(copies.start(sy.at[j, :, (px + k) % N], ry.at[j, k], device(dz=j, dx=k)))

    def relays(o):
        relay("x", o)
        relay("z", o)

    lax.fori_loop(0, 3, bricks(lambda i: i - 1), 0)
    pl.semaphore_wait(barrier, 1 + len(lines))
    for peer in lines:
        pl.semaphore_signal(ready_sem, inc=1, device_id=peer, device_id_type=MESH)
    send_pair(2)
    lax.fori_loop(3, 5, bricks(lambda i: i - 1), 0)
    send_pair(3)
    combine(2)
    lax.fori_loop(5, 7, bricks(lambda i: 8 - i), 0)
    send_pair(1)
    relays(2)
    combine(3)
    lax.fori_loop(7, 8, bricks(lambda i: i - 5), 0)
    send_pair(0)
    combine(1)
    relays(3)
    pl.semaphore_wait(ready_sem, len(lines))
    owners(2)
    combine(0)
    relays(1)
    owners(3)
    owners_y()
    relays(0)
    owners(1)
    owners(0)
    for copy in last:
        copy.wait_recv()

    def total(own, r):
        for j in range(N):
            for k in range(N):
                if (j, k) != (0, 0):
                    own = own + r[j, k]
        return own

    planes = jnp.concatenate([total(sx[0, 0], rx), total(sy[0, :, px], ry), total(sz[0, :, px], rz)], 0)
    rhs_ref[...] = planes[:BX]
    screen_ref[...] = planes[BX:]
    copies.finish()


def splat(first, q, start):
    vm = pl.BlockSpec(memory_space=pltpu.VMEM)
    f32 = jnp.float32
    nx, ny, nz = PARTS
    tile = (BY, BZ)
    made = N * N + 2 * 6 * N + 6 + 45
    shapes = ([(N, 2, 2, nx) + tile] * 4 + [(1, 2, 2, ny, N) + tile] * 4 + [(N, 2, nz, 2) + tile] * 4
              + [(N, N, nx) + tile, (N, ny, N) + tile, (N, nz, N) + tile]
              + [(N, N, nx) + tile, (N, N, ny) + tile, (N, N, nz) + tile])
    return pl.pallas_call(
        splat_kernel,
        out_shape=[jax.ShapeDtypeStruct((BX, BY, BZ), f32)] * 2,
        in_specs=[pl.BlockSpec(memory_space=pltpu.SMEM), vm, vm],
        out_specs=[vm, vm],
        scratch_shapes=[
            pltpu.VMEM((2 * PX * PY, BZ), f32),
            pltpu.VMEM((N, N, 2, BX, N * BY, BZ), f32),
            pltpu.VMEM((N, N, 2 * BX, N) + tile, f32),
            *[pltpu.VMEM(shape, f32) for shape in shapes],
            pltpu.SemaphoreType.DMA((made,)),
            pltpu.SemaphoreType.DMA((made,)),
            pltpu.SemaphoreType.REGULAR,
        ],
        compiler_params=pltpu.CompilerParams(collective_id=0, has_side_effects=True, vmem_limit_bytes=28 << 20),
        name="splat",
    )(first, q, start)


def shards(brick_ids, voxel_offset, fractions, normals, point_weight, tile_count):
    grid, q, first = prepare(brick_ids[:, 0], tile_count, voxel_offset, fractions, normals, point_weight)
    return tuple(splat(first, q, grid))


def solution(mesh):
    return jax.shard_map(
        shards,
        mesh=mesh,
        in_specs=(
            P(("gx", "yz"), None),
            P(("gx", "yz"), None),
            P(("gx", "yz"), None, None),
            P(("gx", "yz"), None, None),
            P(("gx", "yz"), None),
            P(("gx", "yz")),
        ),
        out_specs=(P("gx", "yz", None), P("gx", "yz", None)),
        check_vma=False,
    )
```

```python
import jax
import jax.numpy as jnp
from jax import lax
from jax.experimental import pallas as pl
from jax.experimental.pallas import tpu as pltpu
from jax.sharding import PartitionSpec as P

BX, BY, BZ = 4, 8, 128
PX, PY = 36, 152
V = 8

CZ, WZ, GZ = 0, 3, 6
WY, GY = 9, 19
PXX, PXY, PXZ, PXS = 29, 37, 45, 53
HALF = 61
ROWS = 123
NONE = 128


def spline(f):
    return ((0.5 * (1.0 - f) ** 2, 0.75 - (f - 0.5) ** 2, 0.5 * f * f),
            (f - 1.0, 1.0 - 2.0 * f, f))


def slots(cell, cells, values):
    hit = [cell == c for c in range(cells)]
    out = []
    for i in range(cells + 2):
        total = 0.0
        for k in range(3):
            if 0 <= i - k < cells:
                total = jnp.where(hit[i - k], values[k], total)
        out.append(total)
    return out


def tile_build(t, q_ref):
    parts = [half_build(t * ROWS + h * HALF, q_ref) for h in range(2)]
    return tuple(jnp.concatenate(p, 1) for p in zip(*parts))


def half_build(base, q_ref):
    def row(k):
        return q_ref[pl.ds(base + k, 8, stride=0), :]

    def rows(k):
        return q_ref[pl.ds(base + k, 8), :]

    def pair(k):
        r = row(k)
        return jnp.concatenate([r, r], 0).astype(jnp.bfloat16)

    sixteen = (16, 128)
    cz = [pair(CZ + k) for k in range(3)]
    wz = [pair(WZ + k) for k in range(3)]
    gz = [pair(GZ + k) for k in range(3)]
    zero = jnp.zeros(sixteen, jnp.bfloat16)
    zb, zd = [], []
    for i in range(BZ // 16):
        at = (lax.broadcasted_iota(jnp.int32, sixteen, 0) + 16 * i).astype(jnp.bfloat16)
        hit = [at == c for c in cz]
        zb.append(jnp.where(hit[0], wz[0], jnp.where(hit[1], wz[1], jnp.where(hit[2], wz[2], zero))))
        zd.append(jnp.where(hit[0], gz[0], jnp.where(hit[1], gz[1], jnp.where(hit[2], gz[2], zero))))
    zb = jnp.concatenate(zb, 0)
    zd = jnp.concatenate(zd, 0)

    wy, gy = rows(WY), rows(GY)
    a12, a3, a_s = [], [], []
    for x in range(BX + 2):
        a12.append(row(PXX + x) * wy + row(PXY + x) * gy)
        a3.append(row(PXZ + x) * wy)
        a_s.append(row(PXS + x) * wy)
    p = [rows(k) for k in (PXX, PXY, PXZ, PXS)]
    for y in (BY, BY + 1):
        w, g = row(WY + y), row(GY + y)
        a12.append(p[0] * w + p[1] * g)
        a3.append(p[2] * w)
        a_s.append(p[3] * w)
    lhs1 = jnp.concatenate(a12 + a_s, 0).astype(jnp.bfloat16)
    lhs2 = jnp.concatenate(a3, 0).astype(jnp.bfloat16)
    return lhs1, lhs2, zb, zd


def contract(lhs1, lhs2, zb, zd):
    nt = (((1,), (1,)), ((), ()))
    r1 = lax.dot_general(lhs1, zb, nt, preferred_element_type=jnp.float32)
    r2 = lax.dot_general(lhs2, zd, nt, preferred_element_type=jnp.float32)
    return r1[:64] + r2, r1[64:]


def add_in(slab, column, res, out_ref):
    x0 = slab * BX
    y0 = column * BY + 7
    for f in range(2):
        base = (f * PX + x0) * PY + y0
        for x in range(BX + 2):
            r = pl.ds(base + x * PY, 8)
            out_ref[r, :] += res[f][8 * x:8 * x + 8]
        for k in range(2):
            r = pl.ds(base + 8 + k, 8, stride=PY)
            out_ref[r, :] += res[f][48 + 8 * k:56 + 8 * k]


def prepare_kernel(count_ref, dest_hbm, off_hbm, frac_hbm, norm_hbm, s_hbm, grid_ref, q_ref, first_ref,
                   dest_ref, off_ref, frac_ref, norm_ref, s_ref, list_ref, sems):
    pairs = ((dest_hbm, dest_ref), (off_hbm, off_ref), (frac_hbm, frac_ref), (norm_hbm, norm_ref),
             (s_hbm, s_ref))
    loads = [pltpu.make_async_copy(src, dst, sems.at[i]) for i, (src, dst) in enumerate(pairs)]
    for load in loads:
        load.start()
    grid_ref[...] = jnp.zeros_like(grid_ref)
    q_ref[pl.ds(NONE * ROWS, 128), :] = jnp.zeros((128, 128), jnp.float32)

    def clear(i, _):
        for k in range(8):
            first_ref[i * 8 + k] = NONE
        return 0

    lax.fori_loop(0, NONE // 8, clear, 0)
    for load in loads:
        load.wait()
    count = count_ref[0]

    def group(g, seconds):
        r = pl.ds(pl.multiple_of(g * 8, 8), 8)
        valid = g * 8 + lax.broadcasted_iota(jnp.int32, (8, 128), 0) < count
        for h in range(2):
            lanes = slice(h * 128, h * 128 + 128)

            def put(k, value):
                q_ref[pl.ds(g * 8 * ROWS + h * HALF + k, 8, stride=ROWS), :] = value

            off = off_ref[r, lanes]
            nx, ny, nz = (jnp.where(valid, norm_ref[k, r, lanes], 0.0) for k in range(3))
            s = jnp.where(valid, s_ref[r, lanes], 0.0)
            cell = off & (BZ - 1)
            w, slope = spline(frac_ref[2, r, lanes])
            for k in range(3):
                put(CZ + k, (cell + (k - 1)).astype(jnp.float32))
                put(WZ + k, w[k])
                put(GZ + k, slope[k])
            w, slope = spline(frac_ref[1, r, lanes])
            cell = (off >> 7) & (BY - 1)
            for base, values in ((WY, w), (GY, slope)):
                for i, value in enumerate(slots(cell, BY, values)):
                    put(base + i, value)
            w, slope = spline(frac_ref[0, r, lanes])
            cell = off >> 10
            wx, gx = slots(cell, BX, w), slots(cell, BX, slope)
            for i in range(BX + 2):
                put(PXX + i, nx * gx[i])
                put(PXY + i, ny * wx[i])
                put(PXZ + i, nz * wx[i])
                put(PXS + i, s * wx[i])
            none = jnp.zeros((8, 128), jnp.float32)
            for base in (PXX, PXY, PXZ, PXS):
                put(base + BX + 2, none)
                put(base + BX + 3, none)
        for k in range(8):
            t = g * 8 + k
            brick = dest_ref[t]
            known = first_ref[brick]
            real = t < count
            again = jnp.logical_and(real, known < NONE)
            first_ref[brick] = jnp.where(jnp.logical_and(real, known == NONE), t, known)
            list_ref[seconds] = t
            seconds = seconds + again.astype(jnp.int32)
        return seconds

    seconds = lax.fori_loop(0, NONE // 8, group, 0)
    for k in range(V):
        list_ref[seconds + k] = NONE

    def more(i, _):
        ts = [list_ref[i * V + u] for u in range(V)]
        sums = [contract(*tile_build(t, q_ref)) for t in ts]
        for t, each in zip(ts, sums):
            brick = dest_ref[jnp.minimum(t, NONE - 1)]
            add_in(brick // 16, brick % 16, each, grid_ref)
        return 0

    lax.fori_loop(0, (seconds + V - 1) // V, more, 0)


def prepare(dest, count, off, frac, norm, s):
    tiles, n = off.shape
    hbm = pl.BlockSpec(memory_space=pltpu.HBM)
    f32 = jnp.float32
    return pl.pallas_call(
        prepare_kernel,
        out_shape=[jax.ShapeDtypeStruct((2 * PX * PY, BZ), f32), jax.ShapeDtypeStruct((NONE * ROWS + 128, 128), f32),
                   jax.ShapeDtypeStruct((tiles,), jnp.int32)],
        in_specs=[pl.BlockSpec(memory_space=pltpu.SMEM)] + [hbm] * 5,
        out_specs=[pl.BlockSpec(memory_space=pltpu.VMEM)] * 2 + [pl.BlockSpec(memory_space=pltpu.SMEM)],
        scratch_shapes=[
            pltpu.SMEM((tiles,), jnp.int32), pltpu.VMEM((tiles, n), jnp.int32),
            pltpu.VMEM((3, tiles, n), f32), pltpu.VMEM((3, tiles, n), f32), pltpu.VMEM((tiles, n), f32),
            pltpu.SMEM((tiles + 2 * V,), jnp.int32), pltpu.SemaphoreType.DMA((5,)),
        ],
        compiler_params=pltpu.CompilerParams(vmem_limit_bytes=22 << 20),
        name="prepare",
    )(count, *(pltpu.with_memory_space_constraint(x, pltpu.HBM) for x in
               (dest, off, jnp.transpose(frac, (1, 0, 2)), jnp.transpose(norm, (1, 0, 2)), s)))


N = 4
MESH = pl.DeviceIdType.MESH


class Copies:
    def __init__(self, send_sems, recv_sems):
        self.send_sems, self.recv_sems = send_sems, recv_sems
        self.made = {}

    def start(self, key, where):
        self.made[key] = (len(self.made), where)
        self.copy(key).start()

    def copy(self, key):
        i, where = self.made[key]
        src, dst, device = where()
        return pltpu.make_async_remote_copy(
            src_ref=src, dst_ref=dst, send_sem=self.send_sems.at[i], recv_sem=self.recv_sems.at[i],
            device_id=device, device_id_type=MESH)

    def arrived(self, key):
        self.copy(key).wait_recv()

    def finish(self):
        for key in self.made:
            self.copy(key).wait_send()


DIRECT = (0,)
PARTS = (3, 3, 2)


def splat_kernel(first_ref, q_ref, start_ref, rhs_ref, screen_ref, grid_ref, pair_ref, sum_ref,
                 xa, xb, xc, xr, ya, yb, yc, yr, za, zb, zc, zr, xd, zd, sx, sy, sz, rx, ry, rz, send_sems, recv_sems, ready_sem):
    slab, column = lax.axis_index("gx"), lax.axis_index("yz")
    pz, core = slab // 2, slab % 2
    py, px = column // N, column % N

    def device(dz=0, dy=0, dx=0):
        return (((pz + dz) % N) * 2 + core, ((py + dy) % N) * N + (px + dx) % N)

    other = (pz * 2 + 1 - core, column)
    lines = [device(**{axis: k}) for axis in ("dz", "dy", "dx") for k in range(1, N)]
    barrier = pltpu.get_barrier_semaphore()
    for peer in [other] + lines:
        pl.semaphore_signal(barrier, inc=1, device_id=peer, device_id_type=MESH)

    def fetch(i, _):
        r = pl.ds(pl.multiple_of(i * 96, 96), 96)
        grid_ref[r, :] = start_ref[r, :]
        return 0

    lax.fori_loop(0, 2 * PX * PY // 96, fetch, 0)

    copies = Copies(send_sems, recv_sems)
    grid = grid_ref.reshape(2, PX, PY, BZ)
    def rows_of(o):
        return pl.ds(pl.multiple_of(BY + N * BY * ((py + o) % N), BY), N * BY)

    def cells_of(j, which):
        return 1 + BX * (((pz + j) % N) * 2 + which)

    def send_pair(o):
        for j in range(N):
            copies.start(("pair", o, j), lambda j=j: (
                grid.at[:, pl.ds(cells_of(j, 1 - core), BX), rows_of(o), :], pair_ref.at[o, j], other))

    nx, ny, nz = PARTS
    xs, ys, zs = slice(0, nx), slice(nx, nx + ny), slice(nx + ny, nx + ny + nz)

    def half_of(h):
        return slice(0, N) if h == 2 else slice(2 * h, 2 * h + 2)

    def data(name, o, h, d):
        if name == "x":
            return (o, half_of(h), xs, (px + d) % N)
        if name == "y":
            return (d % N, half_of(h), ys)
        return (o, d % N, zs, half_of(h))

    buffers = {"x": (xa, xb, xc, xr), "y": (ya, yb, yc, yr), "z": (za, zb, zc, zr)}
    straight = {"x": xd, "z": zd}

    def along(name, d):
        return device(**{"d" + name: d})

    def toward(name, way):
        return along(name, 1 if way == 0 else N - 1)

    def send_far(name, o):
        for way in range(2):
            copies.start(("a", name, o, way), lambda way=way: (
                sum_ref.at[data(name, o, way, 2)], buffers[name][0].at[o, way], toward(name, way)))

    def send_near(name, o, ways=(0, 1)):
        for way in ways:
            copies.start(("b", name, o, way), lambda way=way: (
                sum_ref.at[data(name, o, 1 - way, 1 if way == 0 else N - 1)], buffers[name][1].at[o, way],
                toward(name, way)))

    def relay(name, o, ways=(0, 1)):
        a, _, _, r = buffers[name]
        for way in ways:
            copies.arrived(("a", name, o, way))
            r[o, way] = a[o, way] + sum_ref[data(name, o, way, 1 if way == 0 else N - 1)]
            copies.start(("c", name, o, way), lambda way=way: (
                buffers[name][3].at[o, way], buffers[name][2].at[o, way], toward(name, way)))

    def send_straight(name, o):
        for d in (2, 1, 3):
            copies.start(("d", name, o, d), lambda d=d: (
                sum_ref.at[data(name, o, 2, d)], straight[name].at[DIRECT.index(o), d - 1], along(name, d)))

    def combine(o):
        for j in range(N):
            copies.arrived(("pair", o, j))

        def add(j, _):
            for f in range(2):
                for x in range(BX):
                    total = grid[f, cells_of(j, core) + x, rows_of(o), :] + pair_ref[o, j, f, x]
                    sum_ref[o, j, BX * f + x] = total.reshape(N, BY, BZ)
            return 0

        lax.fori_loop(0, N, add, 0)
        if o in DIRECT:
            send_straight("x", o)
            send_straight("z", o)
        else:
            send_far("x", o)
            send_far("z", o)
        if o == 2:
            send_far("y", 0)
        if o not in DIRECT:
            send_near("x", o)
            send_near("z", o)
        if o == 3:
            relay("y", 0, (1,))
            send_near("y", 0, (1,))
        if o == 1:
            relay("y", 0, (0,))
            send_near("y", 0, (0,))

    def joined(name, o, h):
        if o in DIRECT and name != "y":
            half = (half_of(h),) if name == "x" else (slice(None), half_of(h))
            total = sum_ref[data(name, o, h, 0)]
            for d in range(1, N):
                total = total + straight[name][(DIRECT.index(o), d - 1) + half]
            return total
        _, b, c, _ = buffers[name]
        return sum_ref[data(name, o, h, 0)] + c[o, h] + b[o, 1 - h]

    def settle(name, o):
        if o in DIRECT and name != "y":
            for d in range(1, N):
                copies.arrived(("d", name, o, d))
        else:
            for way in range(2):
                copies.arrived(("b", name, o, way))
                copies.arrived(("c", name, o, way))

    last = []

    def start_last(key, where):
        copies.start(key, where)
        last.append(key)

    def owners(o):
        for name, s in (("x", sx), ("z", sz)):
            settle(name, o)
            for h in range(2):
                if name == "x":
                    s[o, half_of(h)] = joined(name, o, h)
                else:
                    s[o, :, half_of(h)] = joined(name, o, h)
            for k in (2, 1, 3, 0):
                if (o, k) != (0, 0):
                    if name == "x":
                        start_last(("last x", o, k), lambda k=k: (sx.at[o, k], rx.at[o, k], device(dy=o, dz=k)))
                    else:
                        start_last(("last z", o, k), lambda k=k: (sz.at[o, :, (px + k) % N], rz.at[o, k], device(dy=o, dx=k)))

    def owners_y():
        settle("y", 0)
        for h in range(2):
            sy[half_of(h)] = joined("y", 0, h)
        for j in (2, 1, 3, 0):
            for k in (2, 1, 3, 0):
                if (j, k) != (0, 0):
                    start_last(("last y", j, k), lambda j=j, k=k: (sy.at[j, :, (px + k) % N], ry.at[j, k], device(dz=j, dx=k)))

    def relays(o):
        if o not in DIRECT:
            relay("x", o)
            relay("z", o)

    def bricks(i, _):
        ys = []
        for k in range(2):
            at = 2 * i + k
            late, latest = at // 10, at // 14
            place = (1 - late) * (at - 1) + (late - latest) * (8 - at) + latest * (at - 5)
            ys.append((N * py + 2 * N + N * N + place) % (N * N))
        places = [(x, y) for y in ys for x in range(2 * N)]
        sums = [contract(*tile_build(first_ref[x * 16 + y], q_ref)) for x, y in places]
        for (x, y), each in zip(places, sums):
            add_in(x, y, each, grid_ref)

        @pl.when(i == 2)
        def _():
            pl.semaphore_wait(barrier, 1 + len(lines))
            for peer in lines:
                pl.semaphore_signal(ready_sem, inc=1, device_id=peer, device_id_type=MESH)
            send_pair(2)

        @pl.when(i == 4)
        def _():
            send_pair(3)
            combine(2)

        @pl.when(i == 6)
        def _():
            send_pair(1)
            relays(2)
            combine(3)
        return 0

    lax.fori_loop(0, 8, bricks, 0)
    send_pair(0)
    combine(1)
    relays(3)
    pl.semaphore_wait(ready_sem, len(lines))
    owners(2)
    combine(0)
    relays(1)
    owners(3)
    owners_y()
    relays(0)
    owners(1)
    owners(0)
    for key in last:
        copies.arrived(key)

    def total(own, r):
        for j in range(N):
            for k in range(N):
                if (j, k) != (0, 0):
                    own = own + r[j, k]
        return own

    planes = jnp.concatenate([total(sx[0, 0], rx), total(sy[0, :, px], ry), total(sz[0, :, px], rz)], 0)
    rhs_ref[...] = planes[:BX]
    screen_ref[...] = planes[BX:]
    copies.finish()


def splat(first, q, start):
    vm = pl.BlockSpec(memory_space=pltpu.VMEM)
    f32 = jnp.float32
    nx, ny, nz = PARTS
    tile = (BY, BZ)
    made = N * N + 2 * 6 * N + 6 + 45
    straight = max(1, len(DIRECT))
    shapes = ([(N, 2, 2, nx) + tile] * 4 + [(1, 2, 2, ny, N) + tile] * 4 + [(N, 2, nz, 2) + tile] * 4
              + [(straight, N - 1, N, nx) + tile, (straight, N - 1, nz, N) + tile]
              + [(N, N, nx) + tile, (N, ny, N) + tile, (N, nz, N) + tile]
              + [(N, N, nx) + tile, (N, N, ny) + tile, (N, N, nz) + tile])
    return pl.pallas_call(
        splat_kernel,
        out_shape=[jax.ShapeDtypeStruct((BX, BY, BZ), f32)] * 2,
        in_specs=[pl.BlockSpec(memory_space=pltpu.SMEM), vm, vm],
        out_specs=[vm, vm],
        scratch_shapes=[
            pltpu.VMEM((2 * PX * PY, BZ), f32),
            pltpu.VMEM((N, N, 2, BX, N * BY, BZ), f32),
            pltpu.VMEM((N, N, 2 * BX, N) + tile, f32),
            *[pltpu.VMEM(shape, f32) for shape in shapes],
            pltpu.SemaphoreType.DMA((made,)),
            pltpu.SemaphoreType.DMA((made,)),
            pltpu.SemaphoreType.REGULAR,
        ],
        compiler_params=pltpu.CompilerParams(collective_id=0, has_side_effects=True, vmem_limit_bytes=28 << 20),
        name="splat",
    )(first, q, start)


def shards(brick_ids, voxel_offset, fractions, normals, point_weight, tile_count):
    grid, q, first = prepare(brick_ids[:, 0], tile_count, voxel_offset, fractions, normals, point_weight)
    return tuple(splat(first, q, grid))


def solution(mesh):
    return jax.shard_map(
        shards,
        mesh=mesh,
        in_specs=(
            P(("gx", "yz"), None),
            P(("gx", "yz"), None),
            P(("gx", "yz"), None, None),
            P(("gx", "yz"), None, None),
            P(("gx", "yz"), None),
            P(("gx", "yz")),
        ),
        out_specs=(P("gx", "yz", None), P("gx", "yz", None)),
        check_vma=False,
    )
```

```python
import jax
import jax.numpy as jnp
from jax import lax
from jax.experimental import pallas as pl
from jax.experimental.pallas import tpu as pltpu
from jax.sharding import PartitionSpec as P

BX, BY, BZ = 4, 8, 128
PX, PY = 36, 152
V = 8

CZ, WZ, GZ = 0, 3, 6
WY, GY = 9, 19
PXX, PXY, PXZ, PXS = 29, 37, 45, 53
HALF = 61
ROWS = 123
NONE = 128


def spline(f):
    return ((0.5 * (1.0 - f) ** 2, 0.75 - (f - 0.5) ** 2, 0.5 * f * f),
            (f - 1.0, 1.0 - 2.0 * f, f))


def slots(cell, cells, values):
    hit = [cell == c for c in range(cells)]
    out = []
    for i in range(cells + 2):
        total = 0.0
        for k in range(3):
            if 0 <= i - k < cells:
                total = jnp.where(hit[i - k], values[k], total)
        out.append(total)
    return out


def tile_build(t, q_ref):
    parts = [half_build(t * ROWS + h * HALF, q_ref) for h in range(2)]
    return tuple(jnp.concatenate(p, 1) for p in zip(*parts))


def half_build(base, q_ref):
    def row(k):
        return q_ref[pl.ds(base + k, 8, stride=0), :]

    def rows(k):
        return q_ref[pl.ds(base + k, 8), :]

    def pair(k):
        r = row(k)
        return jnp.concatenate([r, r], 0).astype(jnp.bfloat16)

    sixteen = (16, 128)
    cz = [pair(CZ + k) for k in range(3)]
    wz = [pair(WZ + k) for k in range(3)]
    gz = [pair(GZ + k) for k in range(3)]
    zero = jnp.zeros(sixteen, jnp.bfloat16)
    zb, zd = [], []
    for i in range(BZ // 16):
        at = (lax.broadcasted_iota(jnp.int32, sixteen, 0) + 16 * i).astype(jnp.bfloat16)
        hit = [at == c for c in cz]
        zb.append(jnp.where(hit[0], wz[0], jnp.where(hit[1], wz[1], jnp.where(hit[2], wz[2], zero))))
        zd.append(jnp.where(hit[0], gz[0], jnp.where(hit[1], gz[1], jnp.where(hit[2], gz[2], zero))))
    zb = jnp.concatenate(zb, 0)
    zd = jnp.concatenate(zd, 0)

    wy, gy = rows(WY), rows(GY)
    a12, a3, a_s = [], [], []
    for x in range(BX + 2):
        a12.append(row(PXX + x) * wy + row(PXY + x) * gy)
        a3.append(row(PXZ + x) * wy)
        a_s.append(row(PXS + x) * wy)
    p = [rows(k) for k in (PXX, PXY, PXZ, PXS)]
    for y in (BY, BY + 1):
        w, g = row(WY + y), row(GY + y)
        a12.append(p[0] * w + p[1] * g)
        a3.append(p[2] * w)
        a_s.append(p[3] * w)
    lhs1 = jnp.concatenate(a12 + a_s, 0).astype(jnp.bfloat16)
    lhs2 = jnp.concatenate(a3, 0).astype(jnp.bfloat16)
    return lhs1, lhs2, zb, zd


def contract(lhs1, lhs2, zb, zd):
    nt = (((1,), (1,)), ((), ()))
    r1 = lax.dot_general(lhs1, zb, nt, preferred_element_type=jnp.float32)
    r2 = lax.dot_general(lhs2, zd, nt, preferred_element_type=jnp.float32)
    return r1[:64] + r2, r1[64:]


def add_in(slab, column, res, out_ref):
    x0 = slab * BX
    y0 = column * BY + 7
    for f in range(2):
        base = (f * PX + x0) * PY + y0
        for x in range(BX + 2):
            r = pl.ds(base + x * PY, 8)
            out_ref[r, :] += res[f][8 * x:8 * x + 8]
        for k in range(2):
            r = pl.ds(base + 8 + k, 8, stride=PY)
            out_ref[r, :] += res[f][48 + 8 * k:56 + 8 * k]


def prepare_kernel(count_ref, dest_hbm, off_hbm, frac_hbm, norm_hbm, s_hbm, grid_ref, q_ref, first_out,
                   dest_ref, off_ref, frac_ref, norm_ref, s_ref, list_ref, first_ref, sems):
    pairs = ((dest_hbm, dest_ref), (off_hbm, off_ref), (frac_hbm, frac_ref), (norm_hbm, norm_ref),
             (s_hbm, s_ref))
    loads = [pltpu.make_async_copy(src, dst, sems.at[i]) for i, (src, dst) in enumerate(pairs)]
    for load in loads:
        load.start()
    grid_ref[...] = jnp.zeros_like(grid_ref)
    q_ref[pl.ds(NONE * ROWS, 128), :] = jnp.zeros((128, 128), jnp.float32)

    def clear(i, _):
        for k in range(8):
            first_ref[i * 8 + k] = NONE
        return 0

    lax.fori_loop(0, NONE // 8, clear, 0)
    for load in loads:
        load.wait()
    count = count_ref[0]

    def group(g, seconds):
        r = pl.ds(pl.multiple_of(g * 8, 8), 8)
        valid = g * 8 + lax.broadcasted_iota(jnp.int32, (8, 128), 0) < count
        for h in range(2):
            lanes = slice(h * 128, h * 128 + 128)

            def put(k, value):
                q_ref[pl.ds(g * 8 * ROWS + h * HALF + k, 8, stride=ROWS), :] = value

            off = off_ref[r, lanes]
            nx, ny, nz = (jnp.where(valid, norm_ref[k, r, lanes], 0.0) for k in range(3))
            s = jnp.where(valid, s_ref[r, lanes], 0.0)
            cell = off & (BZ - 1)
            w, slope = spline(frac_ref[2, r, lanes])
            for k in range(3):
                put(CZ + k, (cell + (k - 1)).astype(jnp.float32))
                put(WZ + k, w[k])
                put(GZ + k, slope[k])
            w, slope = spline(frac_ref[1, r, lanes])
            cell = (off >> 7) & (BY - 1)
            for base, values in ((WY, w), (GY, slope)):
                for i, value in enumerate(slots(cell, BY, values)):
                    put(base + i, value)
            w, slope = spline(frac_ref[0, r, lanes])
            cell = off >> 10
            wx, gx = slots(cell, BX, w), slots(cell, BX, slope)
            for i in range(BX + 2):
                put(PXX + i, nx * gx[i])
                put(PXY + i, ny * wx[i])
                put(PXZ + i, nz * wx[i])
                put(PXS + i, s * wx[i])
            none = jnp.zeros((8, 128), jnp.float32)
            for base in (PXX, PXY, PXZ, PXS):
                put(base + BX + 2, none)
                put(base + BX + 3, none)
        for k in range(8):
            t = g * 8 + k
            brick = dest_ref[t]
            known = first_ref[brick]
            real = t < count
            again = jnp.logical_and(real, known < NONE)
            first_ref[brick] = jnp.where(jnp.logical_and(real, known == NONE), t, known)
            list_ref[seconds] = t
            seconds = seconds + again.astype(jnp.int32)
        return seconds

    seconds = lax.fori_loop(0, NONE // 8, group, 0)
    table = pltpu.make_async_copy(first_ref, first_out, sems.at[5])
    table.start()
    for k in range(V):
        list_ref[seconds + k] = NONE

    def more(i, _):
        ts = [list_ref[i * V + u] for u in range(V)]
        sums = [contract(*tile_build(t, q_ref)) for t in ts]
        for t, each in zip(ts, sums):
            brick = dest_ref[jnp.minimum(t, NONE - 1)]
            add_in(brick // 16, brick % 16, each, grid_ref)
        return 0

    lax.fori_loop(0, (seconds + V - 1) // V, more, 0)
    table.wait()


def prepare(dest, count, off, frac, norm, s):
    tiles, n = off.shape
    hbm = pl.BlockSpec(memory_space=pltpu.HBM)
    f32 = jnp.float32
    return pl.pallas_call(
        prepare_kernel,
        out_shape=[jax.ShapeDtypeStruct((2 * PX * PY, BZ), f32), jax.ShapeDtypeStruct((NONE * ROWS + 128, 128), f32),
                   jax.ShapeDtypeStruct((tiles,), jnp.int32)],
        in_specs=[pl.BlockSpec(memory_space=pltpu.SMEM)] + [hbm] * 5,
        out_specs=[pl.BlockSpec(memory_space=pltpu.VMEM)] * 2 + [pl.BlockSpec(memory_space=pl.ANY)],
        scratch_shapes=[
            pltpu.SMEM((tiles,), jnp.int32), pltpu.VMEM((tiles, n), jnp.int32),
            pltpu.VMEM((3, tiles, n), f32), pltpu.VMEM((3, tiles, n), f32), pltpu.VMEM((tiles, n), f32),
            pltpu.SMEM((tiles + 2 * V,), jnp.int32), pltpu.SMEM((tiles,), jnp.int32), pltpu.SemaphoreType.DMA((6,)),
        ],
        compiler_params=pltpu.CompilerParams(vmem_limit_bytes=22 << 20),
        name="prepare",
    )(count, *(pltpu.with_memory_space_constraint(x, pltpu.HBM) for x in
               (dest, off, jnp.transpose(frac, (1, 0, 2)), jnp.transpose(norm, (1, 0, 2)), s)))


N = 4
MESH = pl.DeviceIdType.MESH


class Copies:
    def __init__(self, send_sems, recv_sems):
        self.send_sems, self.recv_sems = send_sems, recv_sems
        self.made = {}

    def start(self, key, where):
        self.made[key] = (len(self.made), where)
        self.copy(key).start()

    def copy(self, key):
        i, where = self.made[key]
        src, dst, device = where()
        return pltpu.make_async_remote_copy(
            src_ref=src, dst_ref=dst, send_sem=self.send_sems.at[i], recv_sem=self.recv_sems.at[i],
            device_id=device, device_id_type=MESH)

    def arrived(self, key):
        self.copy(key).wait_recv()

    def finish(self):
        for key in self.made:
            self.copy(key).wait_send()


DIRECT = (0, 1, 3)
PARTS = (3, 2, 3)


def splat_kernel(first_hbm, q_ref, start_ref, out_ref, grid_ref, pair_ref, sum_ref,
                 xa, xb, xc, xr, ya, yb, yc, yr, za, zb, zc, zr, xd, zd, sx, sy, sz, rx, ry, rz, send_sems, recv_sems, ready_sem, first_ref, table_sem):
    slab, column = lax.axis_index("gx"), lax.axis_index("yz")
    pz, core = slab // 2, slab % 2
    py, px = column // N, column % N

    def device(dz=0, dy=0, dx=0):
        return (((pz + dz) % N) * 2 + core, ((py + dy) % N) * N + (px + dx) % N)

    other = (pz * 2 + 1 - core, column)
    lines = [device(**{axis: k}) for axis in ("dz", "dy", "dx") for k in range(1, N)]
    barrier = pltpu.get_barrier_semaphore()
    for peer in [other] + lines:
        pl.semaphore_signal(barrier, inc=1, device_id=peer, device_id_type=MESH)

    table = pltpu.make_async_copy(first_hbm, first_ref, table_sem)
    table.start()

    def fetch(y):
        for row in range(2 * PX):
            r = pl.ds(pl.multiple_of(row * PY + BY + BY * y, BY), BY)
            grid_ref[r, :] = start_ref[r, :]

    def fetch_first(k, _):
        fetch((N * py + 2 * N + N * N - 2 + k) % (N * N))
        return 0

    lax.fori_loop(0, 4, fetch_first, 0)
    table.wait()

    copies = Copies(send_sems, recv_sems)
    grid = grid_ref.reshape(2, PX, PY, BZ)
    def rows_of(o):
        return pl.ds(pl.multiple_of(BY + N * BY * ((py + o) % N), BY), N * BY)

    def cells_of(j, which):
        return 1 + BX * (((pz + j) % N) * 2 + which)

    def send_pair(o):
        for j in range(N):
            copies.start(("pair", o, j), lambda j=j: (
                grid.at[:, pl.ds(cells_of(j, 1 - core), BX), rows_of(o), :], pair_ref.at[o, j], other))

    nx, ny, nz = PARTS
    xs, ys, zs = slice(0, nx), slice(nx, nx + ny), slice(nx + ny, nx + ny + nz)

    def half_of(h):
        return slice(0, N) if h == 2 else slice(2 * h, 2 * h + 2)

    def data(name, o, h, d):
        if name == "x":
            return (o, half_of(h), xs, (px + d) % N)
        if name == "y":
            return (d % N, half_of(h), ys)
        return (o, d % N, zs, half_of(h))

    buffers = {"x": (xa, xb, xc, xr), "y": (ya, yb, yc, yr), "z": (za, zb, zc, zr)}
    straight = {"x": xd, "z": zd}

    def along(name, d):
        return device(**{"d" + name: d})

    def toward(name, way):
        return along(name, 1 if way == 0 else N - 1)

    def send_far(name, o):
        for way in range(2):
            copies.start(("a", name, o, way), lambda way=way: (
                sum_ref.at[data(name, o, way, 2)], buffers[name][0].at[o, way], toward(name, way)))

    def send_near(name, o, ways=(0, 1)):
        for way in ways:
            copies.start(("b", name, o, way), lambda way=way: (
                sum_ref.at[data(name, o, 1 - way, 1 if way == 0 else N - 1)], buffers[name][1].at[o, way],
                toward(name, way)))

    def relay(name, o, ways=(0, 1)):
        a, _, _, r = buffers[name]
        for way in ways:
            copies.arrived(("a", name, o, way))
            r[o, way] = a[o, way] + sum_ref[data(name, o, way, 1 if way == 0 else N - 1)]
            copies.start(("c", name, o, way), lambda way=way: (
                buffers[name][3].at[o, way], buffers[name][2].at[o, way], toward(name, way)))

    def send_straight(name, o):
        for d in (2, 1, 3):
            copies.start(("d", name, o, d), lambda d=d: (
                sum_ref.at[data(name, o, 2, d)], straight[name].at[DIRECT.index(o), d - 1], along(name, d)))

    def combine(o):
        for j in range(N):
            copies.arrived(("pair", o, j))

        def add(j, _):
            for f in range(2):
                for x in range(BX):
                    total = grid[f, cells_of(j, core) + x, rows_of(o), :] + pair_ref[o, j, f, x]
                    sum_ref[o, j, BX * f + x] = total.reshape(N, BY, BZ)
            return 0

        lax.fori_loop(0, N, add, 0)
        if o in DIRECT:
            send_straight("x", o)
            send_straight("z", o)
        else:
            send_far("x", o)
            send_far("z", o)
        if o == 2:
            send_far("y", 0)
        if o not in DIRECT:
            send_near("x", o)
            send_near("z", o)
        if o == 3:
            relay("y", 0, (1,))
            send_near("y", 0, (1,))
        if o == 1:
            relay("y", 0, (0,))
            send_near("y", 0, (0,))

    def joined(name, o, h):
        if o in DIRECT and name != "y":
            half = (half_of(h),) if name == "x" else (slice(None), half_of(h))
            total = sum_ref[data(name, o, h, 0)]
            for d in range(1, N):
                total = total + straight[name][(DIRECT.index(o), d - 1) + half]
            return total
        _, b, c, _ = buffers[name]
        return sum_ref[data(name, o, h, 0)] + c[o, h] + b[o, 1 - h]

    def settle(name, o):
        if o in DIRECT and name != "y":
            for d in range(1, N):
                copies.arrived(("d", name, o, d))
        else:
            for way in range(2):
                copies.arrived(("b", name, o, way))
                copies.arrived(("c", name, o, way))

    last = []

    def start_last(key, where):
        copies.start(key, where)
        last.append(key)

    def owners(o):
        for name, s in (("x", sx), ("z", sz)):
            settle(name, o)
            for h in range(2):
                if name == "x":
                    s[o, half_of(h)] = joined(name, o, h)
                else:
                    s[o, :, half_of(h)] = joined(name, o, h)
            for k in (2, 1, 3, 0):
                if (o, k) != (0, 0):
                    if name == "x":
                        start_last(("last x", o, k), lambda k=k: (sx.at[o, k], rx.at[o, k], device(dy=o, dz=k)))
                    else:
                        start_last(("last z", o, k), lambda k=k: (sz.at[o, :, (px + k) % N], rz.at[o, k], device(dy=o, dx=k)))

    def owners_y():
        settle("y", 0)
        for h in range(2):
            sy[half_of(h)] = joined("y", 0, h)
        for j in (2, 1, 3, 0):
            for k in (2, 1, 3, 0):
                if (j, k) != (0, 0):
                    start_last(("last y", j, k), lambda j=j, k=k: (sy.at[j, :, (px + k) % N], ry.at[j, k], device(dz=j, dx=k)))

    def relays(o):
        if o not in DIRECT:
            relay("x", o)
            relay("z", o)

    def bricks(i, _):
        back, done = i // 4, i // 6
        for k in range(2):
            place = (1 - back) * (2 + 2 * i) + back * (4 - 2 * i) + k
            fetch((1 - done) * ((N * py + 2 * N + N * N + place) % (N * N)) + done * N * N)
        ys = []
        for k in range(2):
            at = 2 * i + k
            late, latest = at // 10, at // 14
            place = (1 - late) * (at - 1) + (late - latest) * (8 - at) + latest * (at - 5)
            ys.append((N * py + 2 * N + N * N + place) % (N * N))
        places = [(x, y) for y in ys for x in range(2 * N)]
        sums = [contract(*tile_build(first_ref[x * 16 + y], q_ref)) for x, y in places]
        for (x, y), each in zip(places, sums):
            add_in(x, y, each, grid_ref)

        @pl.when(i == 2)
        def _():
            pl.semaphore_wait(barrier, 1 + len(lines))
            for peer in lines:
                pl.semaphore_signal(ready_sem, inc=1, device_id=peer, device_id_type=MESH)
            send_pair(2)

        @pl.when(i == 4)
        def _():
            send_pair(3)
            combine(2)

        @pl.when(i == 6)
        def _():
            send_pair(1)
            relays(2)
            combine(3)
        return 0

    lax.fori_loop(0, 8, bricks, 0)
    send_pair(0)
    combine(1)
    relays(3)
    pl.semaphore_wait(ready_sem, len(lines))
    owners(2)
    combine(0)
    relays(1)
    owners(3)
    owners_y()
    relays(0)
    owners(1)
    owners(0)
    for key in last:
        copies.arrived(key)

    def total(own, r):
        for j in range(N):
            for k in range(N):
                if (j, k) != (0, 0):
                    own = own + r[j, k]
        return own

    planes = jnp.concatenate([total(sx[0, 0], rx), total(sy[0, :, px], ry), total(sz[0, :, px], rz)], 0)
    out_ref[...] = planes
    copies.finish()


def splat(first, q, start):
    vm = pl.BlockSpec(memory_space=pltpu.VMEM)
    f32 = jnp.float32
    nx, ny, nz = PARTS
    tile = (BY, BZ)
    made = N * N + 2 * 6 * N + 6 + 45
    straight = max(1, len(DIRECT))
    shapes = ([(N, 2, 2, nx) + tile] * 4 + [(1, 2, 2, ny, N) + tile] * 4 + [(N, 2, nz, 2) + tile] * 4
              + [(straight, N - 1, N, nx) + tile, (straight, N - 1, nz, N) + tile]
              + [(N, N, nx) + tile, (N, ny, N) + tile, (N, nz, N) + tile]
              + [(N, N, nx) + tile, (N, N, ny) + tile, (N, N, nz) + tile])
    return pl.pallas_call(
        splat_kernel,
        out_shape=jax.ShapeDtypeStruct((2 * BX, BY, BZ), f32),
        in_specs=[pl.BlockSpec(memory_space=pl.ANY), vm, vm],
        out_specs=vm,
        scratch_shapes=[
            pltpu.VMEM((2 * PX * PY, BZ), f32),
            pltpu.VMEM((N, N, 2, BX, N * BY, BZ), f32),
            pltpu.VMEM((N, N, 2 * BX, N) + tile, f32),
            *[pltpu.VMEM(shape, f32) for shape in shapes],
            pltpu.SemaphoreType.DMA((made,)),
            pltpu.SemaphoreType.DMA((made,)),
            pltpu.SemaphoreType.REGULAR,
            pltpu.SMEM((NONE,), jnp.int32),
            pltpu.SemaphoreType.DMA,
        ],
        compiler_params=pltpu.CompilerParams(collective_id=0, has_side_effects=True, vmem_limit_bytes=28 << 20),
        name="splat",
    )(first, q, start)


def part_kernel(planes_ref, rhs_hbm, screen_hbm, sems):
    copies = [pltpu.make_async_copy(planes_ref.at[pl.ds(BX * i, BX)], hbm, sems.at[i])
              for i, hbm in enumerate((rhs_hbm, screen_hbm))]
    for copy in copies:
        copy.start()
    for copy in copies:
        copy.wait()


def part(planes):
    hbm = pl.BlockSpec(memory_space=pltpu.HBM)
    return pl.pallas_call(
        part_kernel,
        out_shape=[jax.ShapeDtypeStruct((BX, BY, BZ), jnp.float32)] * 2,
        in_specs=[pl.BlockSpec(memory_space=pltpu.VMEM)],
        out_specs=[hbm, hbm],
        scratch_shapes=[pltpu.SemaphoreType.DMA((2,))],
        name="part",
    )(planes)


def shards(brick_ids, voxel_offset, fractions, normals, point_weight, tile_count):
    grid, q, first = prepare(brick_ids[:, 0], tile_count, voxel_offset, fractions, normals, point_weight)
    return tuple(part(pltpu.with_memory_space_constraint(splat(first, q, grid), pltpu.VMEM)))


def solution(mesh):
    return jax.shard_map(
        shards,
        mesh=mesh,
        in_specs=(
            P(("gx", "yz"), None),
            P(("gx", "yz"), None),
            P(("gx", "yz"), None, None),
            P(("gx", "yz"), None, None),
            P(("gx", "yz"), None),
            P(("gx", "yz")),
        ),
        out_specs=(P("gx", "yz", None), P("gx", "yz", None)),
        check_vma=False,
    )
```

```python
import jax
import jax.numpy as jnp
from jax import lax
from jax.experimental import pallas as pl
from jax.experimental.pallas import tpu as pltpu
from jax.sharding import PartitionSpec as P

BX, BY, BZ = 4, 8, 128
PX, PY = 36, 152
V = 8

CZ, WZ, GZ = 0, 3, 6
WY, GY = 9, 19
PXX, PXY, PXZ, PXS = 29, 37, 45, 53
HALF = 61
ROWS = 123
NONE = 128


def spline(f):
    return ((0.5 * (1.0 - f) ** 2, 0.75 - (f - 0.5) ** 2, 0.5 * f * f),
            (f - 1.0, 1.0 - 2.0 * f, f))


def slots(cell, cells, values):
    hit = [cell == c for c in range(cells)]
    out = []
    for i in range(cells + 2):
        total = 0.0
        for k in range(3):
            if 0 <= i - k < cells:
                total = jnp.where(hit[i - k], values[k], total)
        out.append(total)
    return out


def tile_build(t, q_ref):
    parts = [half_build(t * ROWS + h * HALF, q_ref) for h in range(2)]
    return tuple(jnp.concatenate(p, 1) for p in zip(*parts))


def half_build(base, q_ref):
    def row(k):
        return q_ref[pl.ds(base + k, 8, stride=0), :]

    def rows(k):
        return q_ref[pl.ds(base + k, 8), :]

    def pair(k):
        r = row(k)
        return jnp.concatenate([r, r], 0).astype(jnp.bfloat16)

    sixteen = (16, 128)
    cz = [pair(CZ + k) for k in range(3)]
    wz = [pair(WZ + k) for k in range(3)]
    gz = [pair(GZ + k) for k in range(3)]
    zero = jnp.zeros(sixteen, jnp.bfloat16)
    zb, zd = [], []
    for i in range(BZ // 16):
        at = (lax.broadcasted_iota(jnp.int32, sixteen, 0) + 16 * i).astype(jnp.bfloat16)
        hit = [at == c for c in cz]
        zb.append(jnp.where(hit[0], wz[0], jnp.where(hit[1], wz[1], jnp.where(hit[2], wz[2], zero))))
        zd.append(jnp.where(hit[0], gz[0], jnp.where(hit[1], gz[1], jnp.where(hit[2], gz[2], zero))))
    zb = jnp.concatenate(zb, 0)
    zd = jnp.concatenate(zd, 0)

    wy, gy = rows(WY), rows(GY)
    a12, a3, a_s = [], [], []
    for x in range(BX + 2):
        a12.append(row(PXX + x) * wy + row(PXY + x) * gy)
        a3.append(row(PXZ + x) * wy)
        a_s.append(row(PXS + x) * wy)
    p = [rows(k) for k in (PXX, PXY, PXZ, PXS)]
    for y in (BY, BY + 1):
        w, g = row(WY + y), row(GY + y)
        a12.append(p[0] * w + p[1] * g)
        a3.append(p[2] * w)
        a_s.append(p[3] * w)
    lhs1 = jnp.concatenate(a12 + a_s, 0).astype(jnp.bfloat16)
    lhs2 = jnp.concatenate(a3, 0).astype(jnp.bfloat16)
    return lhs1, lhs2, zb, zd


def contract(lhs1, lhs2, zb, zd):
    nt = (((1,), (1,)), ((), ()))
    r1 = lax.dot_general(lhs1, zb, nt, preferred_element_type=jnp.float32)
    r2 = lax.dot_general(lhs2, zd, nt, preferred_element_type=jnp.float32)
    return r1[:64] + r2, r1[64:]


def add_in(slab, column, res, out_ref):
    x0 = slab * BX
    y0 = column * BY + 7
    for f in range(2):
        base = (f * PX + x0) * PY + y0
        for x in range(BX + 2):
            r = pl.ds(base + x * PY, 8)
            out_ref[r, :] += res[f][8 * x:8 * x + 8]
        for k in range(2):
            r = pl.ds(base + 8 + k, 8, stride=PY)
            out_ref[r, :] += res[f][48 + 8 * k:56 + 8 * k]


def prepare_kernel(count_ref, dest_hbm, off_hbm, frac_hbm, norm_hbm, s_hbm, grid_ref, q_ref, first_out,
                   dest_ref, off_ref, frac_ref, norm_ref, s_ref, list_ref, first_ref, sems):
    pairs = ((dest_hbm, dest_ref), (off_hbm, off_ref), (frac_hbm, frac_ref), (norm_hbm, norm_ref),
             (s_hbm, s_ref))
    loads = [pltpu.make_async_copy(src, dst, sems.at[i]) for i, (src, dst) in enumerate(pairs)]
    for load in loads:
        load.start()
    grid_ref[...] = jnp.zeros_like(grid_ref)
    q_ref[pl.ds(NONE * ROWS, 128), :] = jnp.zeros((128, 128), jnp.float32)

    def clear(i, _):
        for k in range(8):
            first_ref[i * 8 + k] = NONE
        return 0

    lax.fori_loop(0, NONE // 8, clear, 0)
    for load in loads:
        load.wait()
    count = count_ref[0]

    def group(g, seconds):
        r = pl.ds(pl.multiple_of(g * 8, 8), 8)
        valid = g * 8 + lax.broadcasted_iota(jnp.int32, (8, 128), 0) < count
        for h in range(2):
            lanes = slice(h * 128, h * 128 + 128)

            def put(k, value):
                q_ref[pl.ds(g * 8 * ROWS + h * HALF + k, 8, stride=ROWS), :] = value

            off = off_ref[r, lanes]
            nx, ny, nz = (jnp.where(valid, norm_ref[k, r, lanes], 0.0) for k in range(3))
            s = jnp.where(valid, s_ref[r, lanes], 0.0)
            cell = off & (BZ - 1)
            w, slope = spline(frac_ref[2, r, lanes])
            for k in range(3):
                put(CZ + k, (cell + (k - 1)).astype(jnp.float32))
                put(WZ + k, w[k])
                put(GZ + k, slope[k])
            w, slope = spline(frac_ref[1, r, lanes])
            cell = (off >> 7) & (BY - 1)
            for base, values in ((WY, w), (GY, slope)):
                for i, value in enumerate(slots(cell, BY, values)):
                    put(base + i, value)
            w, slope = spline(frac_ref[0, r, lanes])
            cell = off >> 10
            wx, gx = slots(cell, BX, w), slots(cell, BX, slope)
            for i in range(BX + 2):
                put(PXX + i, nx * gx[i])
                put(PXY + i, ny * wx[i])
                put(PXZ + i, nz * wx[i])
                put(PXS + i, s * wx[i])
            none = jnp.zeros((8, 128), jnp.float32)
            for base in (PXX, PXY, PXZ, PXS):
                put(base + BX + 2, none)
                put(base + BX + 3, none)
        for k in range(8):
            t = g * 8 + k
            brick = dest_ref[t]
            known = first_ref[brick]
            real = t < count
            again = jnp.logical_and(real, known < NONE)
            first_ref[brick] = jnp.where(jnp.logical_and(real, known == NONE), t, known)
            list_ref[seconds] = t
            seconds = seconds + again.astype(jnp.int32)
        return seconds

    seconds = lax.fori_loop(0, NONE // 8, group, 0)
    table = pltpu.make_async_copy(first_ref, first_out, sems.at[5])
    table.start()
    for k in range(V):
        list_ref[seconds + k] = NONE

    def more(i, _):
        ts = [list_ref[i * V + u] for u in range(V)]
        sums = [contract(*tile_build(t, q_ref)) for t in ts]
        for t, each in zip(ts, sums):
            brick = dest_ref[jnp.minimum(t, NONE - 1)]
            add_in(brick // 16, brick % 16, each, grid_ref)
        return 0

    lax.fori_loop(0, (seconds + V - 1) // V, more, 0)
    table.wait()


def prepare(dest, count, off, frac, norm, s):
    tiles, n = off.shape
    hbm = pl.BlockSpec(memory_space=pltpu.HBM)
    f32 = jnp.float32
    return pl.pallas_call(
        prepare_kernel,
        out_shape=[jax.ShapeDtypeStruct((2 * PX * PY, BZ), f32), jax.ShapeDtypeStruct((NONE * ROWS + 128, 128), f32),
                   jax.ShapeDtypeStruct((tiles,), jnp.int32)],
        in_specs=[pl.BlockSpec(memory_space=pltpu.SMEM)] + [hbm] * 5,
        out_specs=[pl.BlockSpec(memory_space=pltpu.VMEM)] * 2 + [pl.BlockSpec(memory_space=pl.ANY)],
        scratch_shapes=[
            pltpu.SMEM((tiles,), jnp.int32), pltpu.VMEM((tiles, n), jnp.int32),
            pltpu.VMEM((3, tiles, n), f32), pltpu.VMEM((3, tiles, n), f32), pltpu.VMEM((tiles, n), f32),
            pltpu.SMEM((tiles + 2 * V,), jnp.int32), pltpu.SMEM((tiles,), jnp.int32), pltpu.SemaphoreType.DMA((6,)),
        ],
        compiler_params=pltpu.CompilerParams(vmem_limit_bytes=22 << 20),
        name="prepare",
    )(count, *(pltpu.with_memory_space_constraint(x, pltpu.HBM) for x in
               (dest, off, jnp.transpose(frac, (1, 0, 2)), jnp.transpose(norm, (1, 0, 2)), s)))


N = 4
MESH = pl.DeviceIdType.MESH


class Copies:
    def __init__(self, send_sems, recv_sems):
        self.send_sems, self.recv_sems = send_sems, recv_sems
        self.made, self.used = {}, 0

    def start(self, key, where):
        self.many(key, 1, lambda i: where())

    def many(self, key, count, where):
        self.made[key] = (self.used, count, where)
        self.used += count
        self.each(key, lambda copy: copy.start())

    def each(self, key, act):
        base, count, where = self.made[key]

        def one(i, _):
            src, dst, device = where(i)
            act(pltpu.make_async_remote_copy(
                src_ref=src, dst_ref=dst, send_sem=self.send_sems.at[base + i], recv_sem=self.recv_sems.at[base + i],
                device_id=device, device_id_type=MESH))
            return 0

        if count == 1:
            one(0, 0)
        else:
            lax.fori_loop(0, count, one, 0)

    def arrived(self, key):
        self.each(key, lambda copy: copy.wait_recv())

    def finish(self):
        for key in self.made:
            self.each(key, lambda copy: copy.wait_send())


DIRECT = (0, 1, 2, 3)
PARTS = (3, 2, 3)


def splat_kernel(first_hbm, q_ref, start_ref, out_ref, grid_ref, pair_ref, sum_ref,
                 xa, xb, xc, xr, ya, yb, yc, yr, za, zb, zc, zr, xd, zd, sx, sy, sz, rx, ry, rz, send_sems, recv_sems, ready_sem, first_ref, table_sem):
    slab, column = lax.axis_index("gx"), lax.axis_index("yz")
    pz, core = slab // 2, slab % 2
    py, px = column // N, column % N

    def device(dz=0, dy=0, dx=0):
        return (((pz + dz) % N) * 2 + core, ((py + dy) % N) * N + (px + dx) % N)

    other = (pz * 2 + 1 - core, column)
    lines = [device(**{axis: k}) for axis in ("dz", "dy", "dx") for k in range(1, N)]
    barrier = pltpu.get_barrier_semaphore()
    for peer in [other] + lines:
        pl.semaphore_signal(barrier, inc=1, device_id=peer, device_id_type=MESH)

    table = pltpu.make_async_copy(first_hbm, first_ref, table_sem)
    table.start()

    def fetch(y):
        for row in range(2 * PX):
            r = pl.ds(pl.multiple_of(row * PY + BY + BY * y, BY), BY)
            grid_ref[r, :] = start_ref[r, :]

    def fetch_first(k, _):
        fetch((N * py + 2 * N + N * N - 2 + k) % (N * N))
        return 0

    lax.fori_loop(0, 4, fetch_first, 0)
    table.wait()

    copies = Copies(send_sems, recv_sems)
    grid = grid_ref.reshape(2, PX, PY, BZ)
    def rows_of(o):
        return pl.ds(pl.multiple_of(BY + N * BY * ((py + o) % N), BY), N * BY)

    def cells_of(j, which):
        return 1 + BX * (((pz + j) % N) * 2 + which)

    def send_pair(o):
        copies.many(("pair", o), N, lambda j: (
            grid.at[:, pl.ds(cells_of(j, 1 - core), BX), rows_of(o), :], pair_ref.at[o, j], other))

    nx, ny, nz = PARTS
    xs, ys, zs = slice(0, nx), slice(nx, nx + ny), slice(nx + ny, nx + ny + nz)

    def half_of(h):
        return slice(0, N) if h == 2 else slice(2 * h, 2 * h + 2)

    def data(name, o, h, d):
        if name == "x":
            return (o, half_of(h), xs, (px + d) % N)
        if name == "y":
            return (d % N, half_of(h), ys)
        return (o, d % N, zs, half_of(h))

    buffers = {"x": (xa, xb, xc, xr), "y": (ya, yb, yc, yr), "z": (za, zb, zc, zr)}
    straight = {"x": xd, "z": zd}

    def along(name, d):
        return device(**{"d" + name: d})

    def toward(name, way):
        return along(name, 1 if way == 0 else N - 1)

    def send_far(name, o):
        for way in range(2):
            copies.start(("a", name, o, way), lambda way=way: (
                sum_ref.at[data(name, o, way, 2)], buffers[name][0].at[o, way], toward(name, way)))

    def send_near(name, o, ways=(0, 1)):
        for way in ways:
            copies.start(("b", name, o, way), lambda way=way: (
                sum_ref.at[data(name, o, 1 - way, 1 if way == 0 else N - 1)], buffers[name][1].at[o, way],
                toward(name, way)))

    def relay(name, o, ways=(0, 1)):
        a, _, _, r = buffers[name]
        for way in ways:
            copies.arrived(("a", name, o, way))
            r[o, way] = a[o, way] + sum_ref[data(name, o, way, 1 if way == 0 else N - 1)]
            copies.start(("c", name, o, way), lambda way=way: (
                buffers[name][3].at[o, way], buffers[name][2].at[o, way], toward(name, way)))

    def send_straight(name, o):
        def where(i):
            d = (i + 1) % (N - 1) + 1
            return sum_ref.at[data(name, o, 2, d)], straight[name].at[DIRECT.index(o), d - 1], along(name, d)

        copies.many(("d", name, o), N - 1, where)

    def combine(o):
        copies.arrived(("pair", o))

        def add(j, _):
            for f in range(2):
                for x in range(BX):
                    total = grid[f, cells_of(j, core) + x, rows_of(o), :] + pair_ref[o, j, f, x]
                    sum_ref[o, j, BX * f + x] = total.reshape(N, BY, BZ)
            return 0

        lax.fori_loop(0, N, add, 0)
        if o in DIRECT:
            send_straight("x", o)
            send_straight("z", o)
        else:
            send_far("x", o)
            send_far("z", o)
        if o == 2:
            send_far("y", 0)
        if o not in DIRECT:
            send_near("x", o)
            send_near("z", o)
        if o == 3:
            relay("y", 0, (1,))
            send_near("y", 0, (1,))
        if o == 1:
            relay("y", 0, (0,))
            send_near("y", 0, (0,))

    def joined(name, o, h):
        if o in DIRECT and name != "y":
            half = (half_of(h),) if name == "x" else (slice(None), half_of(h))
            total = sum_ref[data(name, o, h, 0)]
            for d in range(1, N):
                total = total + straight[name][(DIRECT.index(o), d - 1) + half]
            return total
        _, b, c, _ = buffers[name]
        return sum_ref[data(name, o, h, 0)] + c[o, h] + b[o, 1 - h]

    def settle(name, o):
        if o in DIRECT and name != "y":
            copies.arrived(("d", name, o))
        else:
            for way in range(2):
                copies.arrived(("b", name, o, way))
                copies.arrived(("c", name, o, way))

    last = []

    def send_last(key, first, count, where):
        copies.many(key, count - first, lambda i: where(i + first))
        last.append(key)

    def owners(o):
        for name, s in (("x", sx), ("z", sz)):
            settle(name, o)
            for h in range(2):
                if name == "x":
                    s[o, half_of(h)] = joined(name, o, h)
                else:
                    s[o, :, half_of(h)] = joined(name, o, h)
        send_last(("last x", o), int(o == 0), N, lambda k: (sx.at[o, k], rx.at[o, k], device(dy=o, dz=k)))
        send_last(("last z", o), int(o == 0), N, lambda k: (sz.at[o, :, (px + k) % N], rz.at[o, k], device(dy=o, dx=k)))

    def owners_y():
        settle("y", 0)
        for h in range(2):
            sy[half_of(h)] = joined("y", 0, h)

        def where(i):
            j, k = i // N, i % N
            return sy.at[j, :, (px + k) % N], ry.at[j, k], device(dz=j, dx=k)

        send_last("last y", 1, N * N, where)

    def bricks(i, _):
        back, done = i // 4, i // 6
        for k in range(2):
            place = (1 - back) * (2 + 2 * i) + back * (4 - 2 * i) + k
            fetch((1 - done) * ((N * py + 2 * N + N * N + place) % (N * N)) + done * N * N)
        ys = []
        for k in range(2):
            at = 2 * i + k
            late, latest = at // 10, at // 14
            place = (1 - late) * (at - 1) + (late - latest) * (8 - at) + latest * (at - 5)
            ys.append((N * py + 2 * N + N * N + place) % (N * N))
        places = [(x, y) for y in ys for x in range(2 * N)]
        sums = [contract(*tile_build(first_ref[x * 16 + y], q_ref)) for x, y in places]
        for (x, y), each in zip(places, sums):
            add_in(x, y, each, grid_ref)

        @pl.when(i == 2)
        def _():
            pl.semaphore_wait(barrier, 1 + len(lines))
            for peer in lines:
                pl.semaphore_signal(ready_sem, inc=1, device_id=peer, device_id_type=MESH)
            send_pair(2)

        @pl.when(i == 4)
        def _():
            send_pair(3)
            combine(2)

        @pl.when(i == 6)
        def _():
            send_pair(1)
            combine(3)
        return 0

    lax.fori_loop(0, 8, bricks, 0)
    send_pair(0)
    combine(1)
    pl.semaphore_wait(ready_sem, len(lines))
    combine(0)
    owners(2)
    owners(3)
    owners_y()
    owners(1)
    owners(0)
    for key in last:
        copies.arrived(key)

    def total(own, r):
        for j in range(N):
            for k in range(N):
                if (j, k) != (0, 0):
                    own = own + r[j, k]
        return own

    planes = jnp.concatenate([total(sx[0, 0], rx), total(sy[0, :, px], ry), total(sz[0, :, px], rz)], 0)
    out_ref[...] = planes
    copies.finish()


def splat(first, q, start):
    vm = pl.BlockSpec(memory_space=pltpu.VMEM)
    f32 = jnp.float32
    nx, ny, nz = PARTS
    tile = (BY, BZ)
    made = N * N + 2 * 6 * N + 6 + 45
    straight = max(1, len(DIRECT))
    shapes = ([(N, 2, 2, nx) + tile] * 4 + [(1, 2, 2, ny, N) + tile] * 4 + [(N, 2, nz, 2) + tile] * 4
              + [(straight, N - 1, N, nx) + tile, (straight, N - 1, nz, N) + tile]
              + [(N, N, nx) + tile, (N, ny, N) + tile, (N, nz, N) + tile]
              + [(N, N, nx) + tile, (N, N, ny) + tile, (N, N, nz) + tile])
    return pl.pallas_call(
        splat_kernel,
        out_shape=jax.ShapeDtypeStruct((2 * BX, BY, BZ), f32),
        in_specs=[pl.BlockSpec(memory_space=pl.ANY), vm, vm],
        out_specs=vm,
        scratch_shapes=[
            pltpu.VMEM((2 * PX * PY, BZ), f32),
            pltpu.VMEM((N, N, 2, BX, N * BY, BZ), f32),
            pltpu.VMEM((N, N, 2 * BX, N) + tile, f32),
            *[pltpu.VMEM(shape, f32) for shape in shapes],
            pltpu.SemaphoreType.DMA((made,)),
            pltpu.SemaphoreType.DMA((made,)),
            pltpu.SemaphoreType.REGULAR,
            pltpu.SMEM((NONE,), jnp.int32),
            pltpu.SemaphoreType.DMA,
        ],
        compiler_params=pltpu.CompilerParams(collective_id=0, has_side_effects=True, vmem_limit_bytes=28 << 20),
        name="splat",
    )(first, q, start)


def part_kernel(planes_ref, rhs_hbm, screen_hbm, sems):
    copies = [pltpu.make_async_copy(planes_ref.at[pl.ds(BX * i, BX)], hbm, sems.at[i])
              for i, hbm in enumerate((rhs_hbm, screen_hbm))]
    for copy in copies:
        copy.start()
    for copy in copies:
        copy.wait()


def part(planes):
    hbm = pl.BlockSpec(memory_space=pltpu.HBM)
    return pl.pallas_call(
        part_kernel,
        out_shape=[jax.ShapeDtypeStruct((BX, BY, BZ), jnp.float32)] * 2,
        in_specs=[pl.BlockSpec(memory_space=pltpu.VMEM)],
        out_specs=[hbm, hbm],
        scratch_shapes=[pltpu.SemaphoreType.DMA((2,))],
        name="part",
    )(planes)


def shards(brick_ids, voxel_offset, fractions, normals, point_weight, tile_count):
    grid, q, first = prepare(brick_ids[:, 0], tile_count, voxel_offset, fractions, normals, point_weight)
    return tuple(part(pltpu.with_memory_space_constraint(splat(first, q, grid), pltpu.VMEM)))


def solution(mesh):
    return jax.shard_map(
        shards,
        mesh=mesh,
        in_specs=(
            P(("gx", "yz"), None),
            P(("gx", "yz"), None),
            P(("gx", "yz"), None, None),
            P(("gx", "yz"), None, None),
            P(("gx", "yz"), None),
            P(("gx", "yz")),
        ),
        out_specs=(P("gx", "yz", None), P("gx", "yz", None)),
        check_vma=False,
    )
```

```python
import jax
import jax.numpy as jnp
from jax import lax
from jax.experimental import pallas as pl
from jax.experimental.pallas import tpu as pltpu
from jax.sharding import PartitionSpec as P

BX, BY, BZ = 4, 8, 128
PX, PY = 36, 152
V = 8

CZ, WZ, GZ = 0, 3, 6
WY, GY = 9, 19
PXX, PXY, PXZ, PXS = 29, 37, 45, 53
HALF = 61
ROWS = 123
NONE = 128


def spline(f):
    return ((0.5 * (1.0 - f) ** 2, 0.75 - (f - 0.5) ** 2, 0.5 * f * f),
            (f - 1.0, 1.0 - 2.0 * f, f))


def slots(cell, cells, values):
    hit = [cell == c for c in range(cells)]
    out = []
    for i in range(cells + 2):
        total = 0.0
        for k in range(3):
            if 0 <= i - k < cells:
                total = jnp.where(hit[i - k], values[k], total)
        out.append(total)
    return out


def tile_build(t, q_ref):
    parts = [half_build(t * ROWS + h * HALF, q_ref) for h in range(2)]
    return tuple(jnp.concatenate(p, 1) for p in zip(*parts))


def half_build(base, q_ref):
    def row(k):
        return q_ref[pl.ds(base + k, 8, stride=0), :]

    def rows(k):
        return q_ref[pl.ds(base + k, 8), :]

    def pair(k):
        r = row(k)
        return jnp.concatenate([r, r], 0).astype(jnp.bfloat16)

    sixteen = (16, 128)
    cz = [pair(CZ + k) for k in range(3)]
    wz = [pair(WZ + k) for k in range(3)]
    gz = [pair(GZ + k) for k in range(3)]
    zero = jnp.zeros(sixteen, jnp.bfloat16)
    zb, zd = [], []
    for i in range(BZ // 16):
        at = (lax.broadcasted_iota(jnp.int32, sixteen, 0) + 16 * i).astype(jnp.bfloat16)
        hit = [at == c for c in cz]
        zb.append(jnp.where(hit[0], wz[0], jnp.where(hit[1], wz[1], jnp.where(hit[2], wz[2], zero))))
        zd.append(jnp.where(hit[0], gz[0], jnp.where(hit[1], gz[1], jnp.where(hit[2], gz[2], zero))))
    zb = jnp.concatenate(zb, 0)
    zd = jnp.concatenate(zd, 0)

    wy, gy = rows(WY), rows(GY)
    a12, a3, a_s = [], [], []
    for x in range(BX + 2):
        a12.append(row(PXX + x) * wy + row(PXY + x) * gy)
        a3.append(row(PXZ + x) * wy)
        a_s.append(row(PXS + x) * wy)
    p = [rows(k) for k in (PXX, PXY, PXZ, PXS)]
    for y in (BY, BY + 1):
        w, g = row(WY + y), row(GY + y)
        a12.append(p[0] * w + p[1] * g)
        a3.append(p[2] * w)
        a_s.append(p[3] * w)
    lhs1 = jnp.concatenate(a12 + a_s, 0).astype(jnp.bfloat16)
    lhs2 = jnp.concatenate(a3, 0).astype(jnp.bfloat16)
    return lhs1, lhs2, zb, zd


def contract(lhs1, lhs2, zb, zd):
    nt = (((1,), (1,)), ((), ()))
    r1 = lax.dot_general(lhs1, zb, nt, preferred_element_type=jnp.float32)
    r2 = lax.dot_general(lhs2, zd, nt, preferred_element_type=jnp.float32)
    return r1[:64] + r2, r1[64:]


def add_in(slab, column, res, out_ref):
    x0 = slab * BX
    y0 = column * BY + 7
    for f in range(2):
        base = (f * PX + x0) * PY + y0
        for x in range(BX + 2):
            r = pl.ds(base + x * PY, 8)
            out_ref[r, :] += res[f][8 * x:8 * x + 8]
        for k in range(2):
            r = pl.ds(base + 8 + k, 8, stride=PY)
            out_ref[r, :] += res[f][48 + 8 * k:56 + 8 * k]


def prepare_kernel(count_ref, dest_hbm, off_hbm, frac_hbm, norm_hbm, s_hbm, grid_ref, q_ref, first_out,
                   dest_ref, off_ref, frac_ref, norm_ref, s_ref, list_ref, first_ref, sems):
    pairs = ((dest_hbm, dest_ref), (off_hbm, off_ref), (frac_hbm, frac_ref), (norm_hbm, norm_ref),
             (s_hbm, s_ref))
    loads = [pltpu.make_async_copy(src, dst, sems.at[i]) for i, (src, dst) in enumerate(pairs)]
    for load in loads:
        load.start()
    grid_ref[...] = jnp.zeros_like(grid_ref)
    q_ref[pl.ds(NONE * ROWS, 128), :] = jnp.zeros((128, 128), jnp.float32)

    def clear(i, _):
        for k in range(8):
            first_ref[i * 8 + k] = NONE
        return 0

    lax.fori_loop(0, NONE // 8, clear, 0)
    for load in loads:
        load.wait()
    count = count_ref[0]

    def group(g, seconds):
        r = pl.ds(pl.multiple_of(g * 8, 8), 8)
        valid = g * 8 + lax.broadcasted_iota(jnp.int32, (8, 128), 0) < count
        for h in range(2):
            lanes = slice(h * 128, h * 128 + 128)

            def put(k, value):
                q_ref[pl.ds(g * 8 * ROWS + h * HALF + k, 8, stride=ROWS), :] = value

            off = off_ref[r, lanes]
            nx, ny, nz = (jnp.where(valid, norm_ref[k, r, lanes], 0.0) for k in range(3))
            s = jnp.where(valid, s_ref[r, lanes], 0.0)
            cell = off & (BZ - 1)
            w, slope = spline(frac_ref[2, r, lanes])
            for k in range(3):
                put(CZ + k, (cell + (k - 1)).astype(jnp.float32))
                put(WZ + k, w[k])
                put(GZ + k, slope[k])
            w, slope = spline(frac_ref[1, r, lanes])
            cell = (off >> 7) & (BY - 1)
            for base, values in ((WY, w), (GY, slope)):
                for i, value in enumerate(slots(cell, BY, values)):
                    put(base + i, value)
            w, slope = spline(frac_ref[0, r, lanes])
            cell = off >> 10
            wx, gx = slots(cell, BX, w), slots(cell, BX, slope)
            for i in range(BX + 2):
                put(PXX + i, nx * gx[i])
                put(PXY + i, ny * wx[i])
                put(PXZ + i, nz * wx[i])
                put(PXS + i, s * wx[i])
            none = jnp.zeros((8, 128), jnp.float32)
            for base in (PXX, PXY, PXZ, PXS):
                put(base + BX + 2, none)
                put(base + BX + 3, none)
        for k in range(8):
            t = g * 8 + k
            brick = dest_ref[t]
            known = first_ref[brick]
            real = t < count
            again = jnp.logical_and(real, known < NONE)
            first_ref[brick] = jnp.where(jnp.logical_and(real, known == NONE), t, known)
            list_ref[seconds] = t
            seconds = seconds + again.astype(jnp.int32)
        return seconds

    seconds = lax.fori_loop(0, NONE // 8, group, 0)
    table = pltpu.make_async_copy(first_ref, first_out, sems.at[5])
    table.start()
    for k in range(V):
        list_ref[seconds + k] = NONE

    def more(i, _):
        ts = [list_ref[i * V + u] for u in range(V)]
        sums = [contract(*tile_build(t, q_ref)) for t in ts]
        for t, each in zip(ts, sums):
            brick = dest_ref[jnp.minimum(t, NONE - 1)]
            add_in(brick // 16, brick % 16, each, grid_ref)
        return 0

    lax.fori_loop(0, (seconds + V - 1) // V, more, 0)
    table.wait()


def prepare(dest, count, off, frac, norm, s):
    tiles, n = off.shape
    hbm = pl.BlockSpec(memory_space=pltpu.HBM)
    f32 = jnp.float32
    return pl.pallas_call(
        prepare_kernel,
        out_shape=[jax.ShapeDtypeStruct((2 * PX * PY, BZ), f32), jax.ShapeDtypeStruct((NONE * ROWS + 128, 128), f32),
                   jax.ShapeDtypeStruct((tiles,), jnp.int32)],
        in_specs=[pl.BlockSpec(memory_space=pltpu.SMEM)] + [hbm] * 5,
        out_specs=[pl.BlockSpec(memory_space=pltpu.VMEM)] * 2 + [pl.BlockSpec(memory_space=pl.ANY)],
        scratch_shapes=[
            pltpu.SMEM((tiles,), jnp.int32), pltpu.VMEM((tiles, n), jnp.int32),
            pltpu.VMEM((3, tiles, n), f32), pltpu.VMEM((3, tiles, n), f32), pltpu.VMEM((tiles, n), f32),
            pltpu.SMEM((tiles + 2 * V,), jnp.int32), pltpu.SMEM((tiles,), jnp.int32), pltpu.SemaphoreType.DMA((6,)),
        ],
        compiler_params=pltpu.CompilerParams(vmem_limit_bytes=22 << 20),
        name="prepare",
    )(count, *(pltpu.with_memory_space_constraint(x, pltpu.HBM) for x in
               (dest, off, jnp.transpose(frac, (1, 0, 2)), jnp.transpose(norm, (1, 0, 2)), s)))


N = 4
MESH = pl.DeviceIdType.MESH


class Copies:
    def __init__(self, send_sems, recv_sems):
        self.send_sems, self.recv_sems = send_sems, recv_sems
        self.made, self.used = {}, 0

    def start(self, key, where):
        self.many(key, 1, lambda i: where())

    def many(self, key, count, where):
        self.made[key] = (self.used, count, where)
        self.used += count
        self.each(key, lambda copy: copy.start())

    def each(self, key, act):
        base, count, where = self.made[key]

        def one(i, _):
            src, dst, device = where(i)
            act(pltpu.make_async_remote_copy(
                src_ref=src, dst_ref=dst, send_sem=self.send_sems.at[base + i], recv_sem=self.recv_sems.at[base + i],
                device_id=device, device_id_type=MESH))
            return 0

        if count == 1:
            one(0, 0)
        else:
            lax.fori_loop(0, count, one, 0)

    def arrived(self, key):
        self.each(key, lambda copy: copy.wait_recv())

    def finish(self):
        for key in self.made:
            self.each(key, lambda copy: copy.wait_send())


DIRECT = (0, 1, 2, 3)
PARTS = (3, 2, 3)


def splat_kernel(first_hbm, q_ref, start_ref, out_ref, grid_ref, pair_ref, sum_ref,
                 xa, xb, xc, xr, ya, yb, yc, yr, za, zb, zc, zr, xd, zd, sx, sy, sz, rx, ry, rz, send_sems, recv_sems, ready_sem, first_ref, table_sem):
    slab, column = lax.axis_index("gx"), lax.axis_index("yz")
    pz, core = slab // 2, slab % 2
    py, px = column // N, column % N

    def device(dz=0, dy=0, dx=0):
        return (((pz + dz) % N) * 2 + core, ((py + dy) % N) * N + (px + dx) % N)

    other = (pz * 2 + 1 - core, column)
    lines = [device(**{axis: k}) for axis in ("dz", "dy", "dx") for k in range(1, N)]
    barrier = pltpu.get_barrier_semaphore()
    for peer in [other] + lines:
        pl.semaphore_signal(barrier, inc=1, device_id=peer, device_id_type=MESH)

    table = pltpu.make_async_copy(first_hbm, first_ref, table_sem)
    table.start()

    def fetch(y):
        for row in range(2 * PX):
            r = pl.ds(pl.multiple_of(row * PY + BY + BY * y, BY), BY)
            grid_ref[r, :] = start_ref[r, :]

    def fetch_first(k, _):
        fetch((N * py + 2 * N + N * N - 2 + k) % (N * N))
        return 0

    lax.fori_loop(0, 4, fetch_first, 0)
    table.wait()

    copies = Copies(send_sems, recv_sems)
    grid = grid_ref.reshape(2, PX, PY, BZ)
    def rows_of(o):
        return pl.ds(pl.multiple_of(BY + N * BY * ((py + o) % N), BY), N * BY)

    def cells_of(j, which):
        return 1 + BX * (((pz + j) % N) * 2 + which)

    def send_pair(o):
        copies.many(("pair", o), N, lambda j: (
            grid.at[:, pl.ds(cells_of(j, 1 - core), BX), rows_of(o), :], pair_ref.at[o, j], other))

    nx, ny, nz = PARTS
    xs, ys, zs = slice(0, nx), slice(nx, nx + ny), slice(nx + ny, nx + ny + nz)

    def half_of(h):
        return slice(0, N) if h == 2 else slice(2 * h, 2 * h + 2)

    def data(name, o, h, d):
        if name == "x":
            return (o, half_of(h), xs, (px + d) % N)
        if name == "y":
            return (d % N, half_of(h), ys)
        return (o, d % N, zs, half_of(h))

    buffers = {"x": (xa, xb, xc, xr), "y": (ya, yb, yc, yr), "z": (za, zb, zc, zr)}
    straight = {"x": xd, "z": zd}

    def along(name, d):
        return device(**{"d" + name: d})

    def toward(name, way):
        return along(name, 1 if way == 0 else N - 1)

    def send_far(name, o):
        for way in range(2):
            copies.start(("a", name, o, way), lambda way=way: (
                sum_ref.at[data(name, o, way, 2)], buffers[name][0].at[o, way], toward(name, way)))

    def send_near(name, o, ways=(0, 1)):
        for way in ways:
            copies.start(("b", name, o, way), lambda way=way: (
                sum_ref.at[data(name, o, 1 - way, 1 if way == 0 else N - 1)], buffers[name][1].at[o, way],
                toward(name, way)))

    def relay(name, o, ways=(0, 1)):
        a, _, _, r = buffers[name]
        for way in ways:
            copies.arrived(("a", name, o, way))
            r[o, way] = a[o, way] + sum_ref[data(name, o, way, 1 if way == 0 else N - 1)]
            copies.start(("c", name, o, way), lambda way=way: (
                buffers[name][3].at[o, way], buffers[name][2].at[o, way], toward(name, way)))

    def send_straight(name, o):
        def where(i):
            d = (i + 1) % (N - 1) + 1
            return sum_ref.at[data(name, o, 2, d)], straight[name].at[DIRECT.index(o), d - 1], along(name, d)

        copies.many(("d", name, o), N - 1, where)

    def combine(o):
        copies.arrived(("pair", o))

        def add(j, _):
            for f in range(2):
                for x in range(BX):
                    total = grid[f, cells_of(j, core) + x, rows_of(o), :] + pair_ref[o, j, f, x]
                    sum_ref[o, j, BX * f + x] = total.reshape(N, BY, BZ)
            return 0

        lax.fori_loop(0, N, add, 0)
        if o in DIRECT:
            send_straight("x", o)
            send_straight("z", o)
        else:
            send_far("x", o)
            send_far("z", o)
        if o == 2:
            send_far("y", 0)
        if o not in DIRECT:
            send_near("x", o)
            send_near("z", o)
        if o == 3:
            relay("y", 0, (1,))
            send_near("y", 0, (1,))
        if o == 1:
            relay("y", 0, (0,))
            send_near("y", 0, (0,))

    def joined(name, o, h):
        if o in DIRECT and name != "y":
            half = (half_of(h),) if name == "x" else (slice(None), half_of(h))
            total = sum_ref[data(name, o, h, 0)]
            for d in range(1, N):
                total = total + straight[name][(DIRECT.index(o), d - 1) + half]
            return total
        _, b, c, _ = buffers[name]
        return sum_ref[data(name, o, h, 0)] + c[o, h] + b[o, 1 - h]

    def settle(name, o):
        if o in DIRECT and name != "y":
            copies.arrived(("d", name, o))
        else:
            for way in range(2):
                copies.arrived(("b", name, o, way))
                copies.arrived(("c", name, o, way))

    last = []

    def send_last(key, first, count, where):
        copies.many(key, count - first, lambda i: where(i + first))
        last.append(key)

    def owners(o):
        for name, s in (("x", sx), ("z", sz)):
            settle(name, o)
            for h in range(2):
                if name == "x":
                    s[o, half_of(h)] = joined(name, o, h)
                else:
                    s[o, :, half_of(h)] = joined(name, o, h)
        send_last(("last x", o), int(o == 0), N, lambda k: (sx.at[o, k], rx.at[o, k], device(dy=o, dz=k)))
        send_last(("last z", o), int(o == 0), N, lambda k: (sz.at[o, :, (px + k) % N], rz.at[o, k], device(dy=o, dx=k)))

    def owners_y():
        settle("y", 0)
        for h in range(2):
            sy[half_of(h)] = joined("y", 0, h)

        def where(i):
            j, k = i // N, i % N
            return sy.at[j, :, (px + k) % N], ry.at[j, k], device(dz=j, dx=k)

        send_last("last y", 1, N * N, where)

    def bricks(i, _):
        back, done = i // 4, i // 6
        for k in range(2):
            place = (1 - back) * (2 + 2 * i) + back * (4 - 2 * i) + k
            fetch((1 - done) * ((N * py + 2 * N + N * N + place) % (N * N)) + done * N * N)
        ys = []
        for k in range(2):
            at = 2 * i + k
            late, latest = at // 10, at // 14
            place = (1 - late) * (at - 1) + (late - latest) * (8 - at) + latest * (at - 5)
            ys.append((N * py + 2 * N + N * N + place) % (N * N))
        places = [(x, y) for y in ys for x in range(2 * N)]
        sums = [contract(*tile_build(first_ref[x * 16 + y], q_ref)) for x, y in places]
        for (x, y), each in zip(places, sums):
            add_in(x, y, each, grid_ref)

        @pl.when(i == 2)
        def _():
            pl.semaphore_wait(barrier, 1 + len(lines))
            for peer in lines:
                pl.semaphore_signal(ready_sem, inc=1, device_id=peer, device_id_type=MESH)
            send_pair(2)

        @pl.when(i == 4)
        def _():
            send_pair(3)
            combine(2)

        @pl.when(i == 6)
        def _():
            send_pair(1)
            combine(3)
        return 0

    lax.fori_loop(0, 8, bricks, 0)
    send_pair(0)
    combine(1)
    pl.semaphore_wait(ready_sem, len(lines))
    combine(0)
    owners(2)
    owners(3)
    owners_y()
    owners(1)
    owners(0)
    copies.finish()
    for key in last:
        copies.arrived(key)

    def total(own, r):
        for j in range(N):
            for k in range(N):
                if (j, k) != (0, 0):
                    own = own + r[j, k]
        return own

    planes = jnp.concatenate([total(sx[0, 0], rx), total(sy[0, :, px], ry), total(sz[0, :, px], rz)], 0)
    out_ref[...] = planes


def splat(first, q, start):
    vm = pl.BlockSpec(memory_space=pltpu.VMEM)
    f32 = jnp.float32
    nx, ny, nz = PARTS
    tile = (BY, BZ)
    made = N * N + 2 * 6 * N + 6 + 45
    straight = max(1, len(DIRECT))
    shapes = ([(N, 2, 2, nx) + tile] * 4 + [(1, 2, 2, ny, N) + tile] * 4 + [(N, 2, nz, 2) + tile] * 4
              + [(straight, N - 1, N, nx) + tile, (straight, N - 1, nz, N) + tile]
              + [(N, N, nx) + tile, (N, ny, N) + tile, (N, nz, N) + tile]
              + [(N, N, nx) + tile, (N, N, ny) + tile, (N, N, nz) + tile])
    return pl.pallas_call(
        splat_kernel,
        out_shape=jax.ShapeDtypeStruct((2 * BX, BY, BZ), f32),
        in_specs=[pl.BlockSpec(memory_space=pl.ANY), vm, vm],
        out_specs=vm,
        scratch_shapes=[
            pltpu.VMEM((2 * PX * PY, BZ), f32),
            pltpu.VMEM((N, N, 2, BX, N * BY, BZ), f32),
            pltpu.VMEM((N, N, 2 * BX, N) + tile, f32),
            *[pltpu.VMEM(shape, f32) for shape in shapes],
            pltpu.SemaphoreType.DMA((made,)),
            pltpu.SemaphoreType.DMA((made,)),
            pltpu.SemaphoreType.REGULAR,
            pltpu.SMEM((NONE,), jnp.int32),
            pltpu.SemaphoreType.DMA,
        ],
        compiler_params=pltpu.CompilerParams(collective_id=0, has_side_effects=True, vmem_limit_bytes=28 << 20),
        name="splat",
    )(first, q, start)


def part_kernel(planes_ref, rhs_hbm, screen_hbm, sems):
    copies = [pltpu.make_async_copy(planes_ref.at[pl.ds(BX * i, BX)], hbm, sems.at[i])
              for i, hbm in enumerate((rhs_hbm, screen_hbm))]
    for copy in copies:
        copy.start()
    for copy in copies:
        copy.wait()


def part(planes):
    hbm = pl.BlockSpec(memory_space=pltpu.HBM)
    return pl.pallas_call(
        part_kernel,
        out_shape=[jax.ShapeDtypeStruct((BX, BY, BZ), jnp.float32)] * 2,
        in_specs=[pl.BlockSpec(memory_space=pltpu.VMEM)],
        out_specs=[hbm, hbm],
        scratch_shapes=[pltpu.SemaphoreType.DMA((2,))],
        name="part",
    )(planes)


def shards(brick_ids, voxel_offset, fractions, normals, point_weight, tile_count):
    grid, q, first = prepare(brick_ids[:, 0], tile_count, voxel_offset, fractions, normals, point_weight)
    return tuple(part(pltpu.with_memory_space_constraint(splat(first, q, grid), pltpu.VMEM)))


def solution(mesh):
    return jax.shard_map(
        shards,
        mesh=mesh,
        in_specs=(
            P(("gx", "yz"), None),
            P(("gx", "yz"), None),
            P(("gx", "yz"), None, None),
            P(("gx", "yz"), None, None),
            P(("gx", "yz"), None),
            P(("gx", "yz")),
        ),
        out_specs=(P("gx", "yz", None), P("gx", "yz", None)),
        check_vma=False,
    )
```

```python
import jax
import jax.numpy as jnp
from jax import lax
from jax.experimental import pallas as pl
from jax.experimental.pallas import tpu as pltpu
from jax.sharding import PartitionSpec as P

BX, BY, BZ = 4, 8, 128
PX, PY = 36, 152
V = 8

CZ, WZ, GZ = 0, 3, 6
WY, GY = 9, 19
PXX, PXY, PXZ, PXS = 29, 37, 45, 53
HALF = 61
ROWS = 123
NONE = 128


def spline(f):
    return ((0.5 * (1.0 - f) ** 2, 0.75 - (f - 0.5) ** 2, 0.5 * f * f),
            (f - 1.0, 1.0 - 2.0 * f, f))


def slots(cell, cells, values):
    hit = [cell == c for c in range(cells)]
    out = []
    for i in range(cells + 2):
        total = 0.0
        for k in range(3):
            if 0 <= i - k < cells:
                total = jnp.where(hit[i - k], values[k], total)
        out.append(total)
    return out


def tile_build(t, q_ref):
    parts = [half_build(t * ROWS + h * HALF, q_ref) for h in range(2)]
    return tuple(jnp.concatenate(p, 1) for p in zip(*parts))


def half_build(base, q_ref):
    def row(k):
        return q_ref[pl.ds(base + k, 8, stride=0), :]

    def rows(k):
        return q_ref[pl.ds(base + k, 8), :]

    def pair(k):
        r = row(k)
        return jnp.concatenate([r, r], 0).astype(jnp.bfloat16)

    sixteen = (16, 128)
    cz = [pair(CZ + k) for k in range(3)]
    wz = [pair(WZ + k) for k in range(3)]
    gz = [pair(GZ + k) for k in range(3)]
    zero = jnp.zeros(sixteen, jnp.bfloat16)
    zb, zd = [], []
    for i in range(BZ // 16):
        at = (lax.broadcasted_iota(jnp.int32, sixteen, 0) + 16 * i).astype(jnp.bfloat16)
        hit = [at == c for c in cz]
        zb.append(jnp.where(hit[0], wz[0], jnp.where(hit[1], wz[1], jnp.where(hit[2], wz[2], zero))))
        zd.append(jnp.where(hit[0], gz[0], jnp.where(hit[1], gz[1], jnp.where(hit[2], gz[2], zero))))
    zb = jnp.concatenate(zb, 0)
    zd = jnp.concatenate(zd, 0)

    wy, gy = rows(WY), rows(GY)
    a12, a3, a_s = [], [], []
    for x in range(BX + 2):
        a12.append(row(PXX + x) * wy + row(PXY + x) * gy)
        a3.append(row(PXZ + x) * wy)
        a_s.append(row(PXS + x) * wy)
    p = [rows(k) for k in (PXX, PXY, PXZ, PXS)]
    for y in (BY, BY + 1):
        w, g = row(WY + y), row(GY + y)
        a12.append(p[0] * w + p[1] * g)
        a3.append(p[2] * w)
        a_s.append(p[3] * w)
    lhs1 = jnp.concatenate(a12 + a_s, 0).astype(jnp.bfloat16)
    lhs2 = jnp.concatenate(a3, 0).astype(jnp.bfloat16)
    return lhs1, lhs2, zb, zd


def contract(lhs1, lhs2, zb, zd):
    nt = (((1,), (1,)), ((), ()))
    r1 = lax.dot_general(lhs1, zb, nt, preferred_element_type=jnp.float32)
    r2 = lax.dot_general(lhs2, zd, nt, preferred_element_type=jnp.float32)
    return r1[:64] + r2, r1[64:]


def add_in(slab, column, res, out_ref):
    x0 = slab * BX
    y0 = column * BY + 7
    for f in range(2):
        base = (f * PX + x0) * PY + y0
        for x in range(BX + 2):
            r = pl.ds(base + x * PY, 8)
            out_ref[r, :] += res[f][8 * x:8 * x + 8]
        for k in range(2):
            r = pl.ds(base + 8 + k, 8, stride=PY)
            out_ref[r, :] += res[f][48 + 8 * k:56 + 8 * k]


def prepare_kernel(count_ref, dest_hbm, off_hbm, frac_hbm, norm_hbm, s_hbm, grid_ref, q_ref, first_out,
                   dest_ref, off_ref, frac_ref, norm_ref, s_ref, list_ref, first_ref, sems):
    pairs = ((dest_hbm, dest_ref), (off_hbm, off_ref), (frac_hbm, frac_ref), (norm_hbm, norm_ref),
             (s_hbm, s_ref))
    loads = [pltpu.make_async_copy(src, dst, sems.at[i]) for i, (src, dst) in enumerate(pairs)]
    for load in loads:
        load.start()
    grid_ref[...] = jnp.zeros_like(grid_ref)
    q_ref[pl.ds(NONE * ROWS, 128), :] = jnp.zeros((128, 128), jnp.float32)

    def clear(i, _):
        for k in range(8):
            first_ref[i * 8 + k] = NONE
        return 0

    lax.fori_loop(0, NONE // 8, clear, 0)
    for load in loads:
        load.wait()
    count = count_ref[0]

    def group(g, seconds):
        r = pl.ds(pl.multiple_of(g * 8, 8), 8)
        valid = g * 8 + lax.broadcasted_iota(jnp.int32, (8, 128), 0) < count
        for h in range(2):
            lanes = slice(h * 128, h * 128 + 128)

            def put(k, value):
                q_ref[pl.ds(g * 8 * ROWS + h * HALF + k, 8, stride=ROWS), :] = value

            off = off_ref[r, lanes]
            nx, ny, nz = (jnp.where(valid, norm_ref[k, r, lanes], 0.0) for k in range(3))
            s = jnp.where(valid, s_ref[r, lanes], 0.0)
            cell = off & (BZ - 1)
            w, slope = spline(frac_ref[2, r, lanes])
            for k in range(3):
                put(CZ + k, (cell + (k - 1)).astype(jnp.float32))
                put(WZ + k, w[k])
                put(GZ + k, slope[k])
            w, slope = spline(frac_ref[1, r, lanes])
            cell = (off >> 7) & (BY - 1)
            for base, values in ((WY, w), (GY, slope)):
                for i, value in enumerate(slots(cell, BY, values)):
                    put(base + i, value)
            w, slope = spline(frac_ref[0, r, lanes])
            cell = off >> 10
            wx, gx = slots(cell, BX, w), slots(cell, BX, slope)
            for i in range(BX + 2):
                put(PXX + i, nx * gx[i])
                put(PXY + i, ny * wx[i])
                put(PXZ + i, nz * wx[i])
                put(PXS + i, s * wx[i])
            none = jnp.zeros((8, 128), jnp.float32)
            for base in (PXX, PXY, PXZ, PXS):
                put(base + BX + 2, none)
                put(base + BX + 3, none)
        for k in range(8):
            t = g * 8 + k
            brick = dest_ref[t]
            known = first_ref[brick]
            real = t < count
            again = jnp.logical_and(real, known < NONE)
            first_ref[brick] = jnp.where(jnp.logical_and(real, known == NONE), t, known)
            list_ref[seconds] = t
            seconds = seconds + again.astype(jnp.int32)
        return seconds

    seconds = lax.fori_loop(0, NONE // 8, group, 0)
    table = pltpu.make_async_copy(first_ref, first_out, sems.at[5])
    table.start()
    for k in range(V):
        list_ref[seconds + k] = NONE

    def more(i, _):
        ts = [list_ref[i * V + u] for u in range(V)]
        sums = [contract(*tile_build(t, q_ref)) for t in ts]
        for t, each in zip(ts, sums):
            brick = dest_ref[jnp.minimum(t, NONE - 1)]
            add_in(brick // 16, brick % 16, each, grid_ref)
        return 0

    lax.fori_loop(0, (seconds + V - 1) // V, more, 0)
    table.wait()


def prepare(dest, count, off, frac, norm, s):
    tiles, n = off.shape
    hbm = pl.BlockSpec(memory_space=pltpu.HBM)
    f32 = jnp.float32
    return pl.pallas_call(
        prepare_kernel,
        out_shape=[jax.ShapeDtypeStruct((2 * PX * PY, BZ), f32), jax.ShapeDtypeStruct((NONE * ROWS + 128, 128), f32),
                   jax.ShapeDtypeStruct((tiles,), jnp.int32)],
        in_specs=[pl.BlockSpec(memory_space=pltpu.SMEM)] + [hbm] * 5,
        out_specs=[pl.BlockSpec(memory_space=pltpu.VMEM)] * 2 + [pl.BlockSpec(memory_space=pl.ANY)],
        scratch_shapes=[
            pltpu.SMEM((tiles,), jnp.int32), pltpu.VMEM((tiles, n), jnp.int32),
            pltpu.VMEM((3, tiles, n), f32), pltpu.VMEM((3, tiles, n), f32), pltpu.VMEM((tiles, n), f32),
            pltpu.SMEM((tiles + 2 * V,), jnp.int32), pltpu.SMEM((tiles,), jnp.int32), pltpu.SemaphoreType.DMA((6,)),
        ],
        compiler_params=pltpu.CompilerParams(vmem_limit_bytes=22 << 20),
        name="prepare",
    )(count, *(pltpu.with_memory_space_constraint(x, pltpu.HBM) for x in
               (dest, off, jnp.transpose(frac, (1, 0, 2)), jnp.transpose(norm, (1, 0, 2)), s)))


N = 4
MESH = pl.DeviceIdType.MESH


class Copies:
    def __init__(self, send_sems, recv_sems):
        self.send_sems, self.recv_sems = send_sems, recv_sems
        self.made, self.used = {}, 0

    def start(self, key, where):
        self.many(key, 1, lambda i: where())

    def many(self, key, count, where):
        self.made[key] = (self.used, count, where)
        self.used += count
        self.each(key, lambda copy: copy.start())

    def each(self, key, act):
        base, count, where = self.made[key]

        def one(i, _):
            src, dst, device = where(i)
            act(pltpu.make_async_remote_copy(
                src_ref=src, dst_ref=dst, send_sem=self.send_sems.at[base + i], recv_sem=self.recv_sems.at[base + i],
                device_id=device, device_id_type=MESH))
            return 0

        if count == 1:
            one(0, 0)
        else:
            lax.fori_loop(0, count, one, 0)

    def arrived(self, key):
        self.each(key, lambda copy: copy.wait_recv())

    def finish(self):
        for key in self.made:
            self.each(key, lambda copy: copy.wait_send())


DIRECT = (0, 1, 2, 3)
PARTS = (3, 2, 3)


def splat_kernel(first_hbm, q_ref, start_ref, out_ref, grid_ref, pair_ref, sum_ref,
                 xa, xb, xc, xr, ya, yb, yc, yr, za, zb, zc, zr, xd, zd, sx, sy, sz, rx, ry, rz, send_sems, recv_sems, ready_sem, first_ref, table_sem):
    slab, column = lax.axis_index("gx"), lax.axis_index("yz")
    pz, core = slab // 2, slab % 2
    py, px = column // N, column % N

    def device(dz=0, dy=0, dx=0):
        return (((pz + dz) % N) * 2 + core, ((py + dy) % N) * N + (px + dx) % N)

    other = (pz * 2 + 1 - core, column)
    lines = [device(**{axis: k}) for axis in ("dz", "dy", "dx") for k in range(1, N)]
    barrier = pltpu.get_barrier_semaphore()
    for peer in [other] + lines:
        pl.semaphore_signal(barrier, inc=1, device_id=peer, device_id_type=MESH)

    table = pltpu.make_async_copy(first_hbm, first_ref, table_sem)
    table.start()

    def fetch(y):
        for row in range(2 * PX):
            r = pl.ds(pl.multiple_of(row * PY + BY + BY * y, BY), BY)
            grid_ref[r, :] = start_ref[r, :]

    def fetch_first(k, _):
        fetch((N * py + 2 * N + N * N - 2 + k) % (N * N))
        return 0

    lax.fori_loop(0, 4, fetch_first, 0)
    table.wait()

    copies = Copies(send_sems, recv_sems)
    grid = grid_ref.reshape(2, PX, PY, BZ)
    def rows_of(o):
        return pl.ds(pl.multiple_of(BY + N * BY * ((py + o) % N), BY), N * BY)

    def cells_of(j, which):
        return 1 + BX * (((pz + j) % N) * 2 + which)

    def send_pair(o):
        copies.many(("pair", o), N, lambda j: (
            grid.at[:, pl.ds(cells_of(j, 1 - core), BX), rows_of(o), :], pair_ref.at[o, j], other))

    nx, ny, nz = PARTS
    xs, ys, zs = slice(0, nx), slice(nx, nx + ny), slice(nx + ny, nx + ny + nz)

    def half_of(h):
        return slice(0, N) if h == 2 else slice(2 * h, 2 * h + 2)

    def data(name, o, h, d):
        if name == "x":
            return (o, half_of(h), xs, (px + d) % N)
        if name == "y":
            return (d % N, half_of(h), ys)
        return (o, d % N, zs, half_of(h))

    buffers = {"x": (xa, xb, xc, xr), "y": (ya, yb, yc, yr), "z": (za, zb, zc, zr)}
    straight = {"x": xd, "z": zd}

    def along(name, d):
        return device(**{"d" + name: d})

    def toward(name, way):
        return along(name, 1 if way == 0 else N - 1)

    def send_far(name, o):
        for way in range(2):
            copies.start(("a", name, o, way), lambda way=way: (
                sum_ref.at[data(name, o, way, 2)], buffers[name][0].at[o, way], toward(name, way)))

    def send_near(name, o, ways=(0, 1)):
        for way in ways:
            copies.start(("b", name, o, way), lambda way=way: (
                sum_ref.at[data(name, o, 1 - way, 1 if way == 0 else N - 1)], buffers[name][1].at[o, way],
                toward(name, way)))

    def relay(name, o, ways=(0, 1)):
        a, _, _, r = buffers[name]
        for way in ways:
            copies.arrived(("a", name, o, way))
            r[o, way] = a[o, way] + sum_ref[data(name, o, way, 1 if way == 0 else N - 1)]
            copies.start(("c", name, o, way), lambda way=way: (
                buffers[name][3].at[o, way], buffers[name][2].at[o, way], toward(name, way)))

    def send_straight(name, o):
        def where(i):
            d = (i + 1) % (N - 1) + 1
            return sum_ref.at[data(name, o, 2, d)], straight[name].at[DIRECT.index(o), d - 1], along(name, d)

        copies.many(("d", name, o), N - 1, where)

    def combine(o):
        copies.arrived(("pair", o))

        def add(j, _):
            for f in range(2):
                for x in range(BX):
                    total = grid[f, cells_of(j, core) + x, rows_of(o), :] + pair_ref[o, j, f, x]
                    sum_ref[o, j, BX * f + x] = total.reshape(N, BY, BZ)
            return 0

        lax.fori_loop(0, N, add, 0)
        if o in DIRECT:
            send_straight("x", o)
            send_straight("z", o)
        else:
            send_far("x", o)
            send_far("z", o)
        if o == 2:
            send_far("y", 0)
        if o not in DIRECT:
            send_near("x", o)
            send_near("z", o)
        if o == 3:
            relay("y", 0, (1,))
            send_near("y", 0, (1,))
        if o == 1:
            relay("y", 0, (0,))
            send_near("y", 0, (0,))

    def joined(name, o, h):
        if o in DIRECT and name != "y":
            half = (half_of(h),) if name == "x" else (slice(None), half_of(h))
            total = sum_ref[data(name, o, h, 0)]
            for d in range(1, N):
                total = total + straight[name][(DIRECT.index(o), d - 1) + half]
            return total
        _, b, c, _ = buffers[name]
        return sum_ref[data(name, o, h, 0)] + c[o, h] + b[o, 1 - h]

    def settle(name, o):
        if o in DIRECT and name != "y":
            copies.arrived(("d", name, o))
        else:
            for way in range(2):
                copies.arrived(("b", name, o, way))
                copies.arrived(("c", name, o, way))

    last = []

    def send_last(key, first, count, ahead, where):
        copies.many(key, count - first, lambda i: where((i + ahead) % (count - first) + first))
        last.append(key)

    def owners(o):
        for name, s in (("x", sx), ("z", sz)):
            settle(name, o)
            for h in range(2):
                if name == "x":
                    s[o, half_of(h)] = joined(name, o, h)
                else:
                    s[o, :, half_of(h)] = joined(name, o, h)
        send_last(("last x", o), int(o == 0), N, 2 - int(o == 0), lambda k: (sx.at[o, k], rx.at[o, k], device(dy=o, dz=k)))
        send_last(("last z", o), int(o == 0), N, 2 - int(o == 0), lambda k: (sz.at[o, :, (px + k) % N], rz.at[o, k], device(dy=o, dx=k)))

    def owners_y():
        settle("y", 0)
        for h in range(2):
            sy[half_of(h)] = joined("y", 0, h)

        def where(i):
            j, k = i // N, i % N
            return sy.at[j, :, (px + k) % N], ry.at[j, k], device(dz=j, dx=k)

        send_last("last y", 1, N * N, 2 * N + 1, where)

    def bricks(i, _):
        back, done = i // 4, i // 6
        for k in range(2):
            place = (1 - back) * (2 + 2 * i) + back * (4 - 2 * i) + k
            fetch((1 - done) * ((N * py + 2 * N + N * N + place) % (N * N)) + done * N * N)
        ys = []
        for k in range(2):
            at = 2 * i + k
            late, latest = at // 10, at // 14
            place = (1 - late) * (at - 1) + (late - latest) * (8 - at) + latest * (at - 5)
            ys.append((N * py + 2 * N + N * N + place) % (N * N))
        places = [(x, y) for y in ys for x in range(2 * N)]
        sums = [contract(*tile_build(first_ref[x * 16 + y], q_ref)) for x, y in places]
        for (x, y), each in zip(places, sums):
            add_in(x, y, each, grid_ref)

        @pl.when(i == 2)
        def _():
            pl.semaphore_wait(barrier, 1 + len(lines))
            for peer in lines:
                pl.semaphore_signal(ready_sem, inc=1, device_id=peer, device_id_type=MESH)
            send_pair(2)

        @pl.when(i == 4)
        def _():
            send_pair(3)
            combine(2)

        @pl.when(i == 6)
        def _():
            send_pair(1)
            combine(3)
        return 0

    lax.fori_loop(0, 8, bricks, 0)
    send_pair(0)
    combine(1)
    pl.semaphore_wait(ready_sem, len(lines))
    combine(0)
    owners(2)
    owners(3)
    owners_y()
    owners(1)
    owners(0)
    copies.finish()
    for key in last:
        copies.arrived(key)

    def total(own, r):
        for j in range(N):
            for k in range(N):
                if (j, k) != (0, 0):
                    own = own + r[j, k]
        return own

    planes = jnp.concatenate([total(sx[0, 0], rx), total(sy[0, :, px], ry), total(sz[0, :, px], rz)], 0)
    out_ref[...] = planes


def splat(first, q, start):
    vm = pl.BlockSpec(memory_space=pltpu.VMEM)
    f32 = jnp.float32
    nx, ny, nz = PARTS
    tile = (BY, BZ)
    made = N * N + 2 * 6 * N + 6 + 45
    straight = max(1, len(DIRECT))
    shapes = ([(N, 2, 2, nx) + tile] * 4 + [(1, 2, 2, ny, N) + tile] * 4 + [(N, 2, nz, 2) + tile] * 4
              + [(straight, N - 1, N, nx) + tile, (straight, N - 1, nz, N) + tile]
              + [(N, N, nx) + tile, (N, ny, N) + tile, (N, nz, N) + tile]
              + [(N, N, nx) + tile, (N, N, ny) + tile, (N, N, nz) + tile])
    return pl.pallas_call(
        splat_kernel,
        out_shape=jax.ShapeDtypeStruct((2 * BX, BY, BZ), f32),
        in_specs=[pl.BlockSpec(memory_space=pl.ANY), vm, vm],
        out_specs=vm,
        scratch_shapes=[
            pltpu.VMEM((2 * PX * PY, BZ), f32),
            pltpu.VMEM((N, N, 2, BX, N * BY, BZ), f32),
            pltpu.VMEM((N, N, 2 * BX, N) + tile, f32),
            *[pltpu.VMEM(shape, f32) for shape in shapes],
            pltpu.SemaphoreType.DMA((made,)),
            pltpu.SemaphoreType.DMA((made,)),
            pltpu.SemaphoreType.REGULAR,
            pltpu.SMEM((NONE,), jnp.int32),
            pltpu.SemaphoreType.DMA,
        ],
        compiler_params=pltpu.CompilerParams(collective_id=0, has_side_effects=True, vmem_limit_bytes=28 << 20),
        name="splat",
    )(first, q, start)


def part_kernel(planes_ref, rhs_hbm, screen_hbm, sems):
    copies = [pltpu.make_async_copy(planes_ref.at[pl.ds(BX * i, BX)], hbm, sems.at[i])
              for i, hbm in enumerate((rhs_hbm, screen_hbm))]
    for copy in copies:
        copy.start()
    for copy in copies:
        copy.wait()


def part(planes):
    hbm = pl.BlockSpec(memory_space=pltpu.HBM)
    return pl.pallas_call(
        part_kernel,
        out_shape=[jax.ShapeDtypeStruct((BX, BY, BZ), jnp.float32)] * 2,
        in_specs=[pl.BlockSpec(memory_space=pltpu.VMEM)],
        out_specs=[hbm, hbm],
        scratch_shapes=[pltpu.SemaphoreType.DMA((2,))],
        name="part",
    )(planes)


def shards(brick_ids, voxel_offset, fractions, normals, point_weight, tile_count):
    grid, q, first = prepare(brick_ids[:, 0], tile_count, voxel_offset, fractions, normals, point_weight)
    return tuple(part(pltpu.with_memory_space_constraint(splat(first, q, grid), pltpu.VMEM)))


def solution(mesh):
    return jax.shard_map(
        shards,
        mesh=mesh,
        in_specs=(
            P(("gx", "yz"), None),
            P(("gx", "yz"), None),
            P(("gx", "yz"), None, None),
            P(("gx", "yz"), None, None),
            P(("gx", "yz"), None),
            P(("gx", "yz")),
        ),
        out_specs=(P("gx", "yz", None), P("gx", "yz", None)),
        check_vma=False,
    )
```
